128 devices in a mesh: gx: 16 (over z, x), gy: 8 (over y, core).
Axes of the slice: x: 4, y: 4, z: 4, core: 2. Of those that a mesh axis runs over, the one named last changes fastest.
Arguments:
- density: float32 [1024, 256, 128], P('gx', 'gy'), may hold values from -6 to 6
- slowness: float32 [1024, 256, 128], P('gx', 'gy'), may hold values from -6 to 6
- pressure_obs: float32 [1024, 256, 128], P('gx', 'gy'), may hold values from -6 to 6
- time_obs: float32 [1024, 256, 128], P('gx', 'gy'), may hold values from -6 to 6
- zone_map: int32 [1024, 256, 128], P('gx', 'gy'), may hold values from 0 to 7
- zone_low: float32 [8], replicated, may hold values from -2.5 to -0.5
- zone_high: float32 [8], replicated, may hold values from 0.5 to 2.5
Outputs:
- density_out: float32 [1024, 256, 128], P('gx', 'gy')
- slowness_out: float32 [1024, 256, 128], P('gx', 'gy')
- objective: float32 [3], replicated
The draws below stay inside these ranges and needn't reach their ends.
All inputs are finite; a program needn't handle non-finite values.
Results may differ from the reference program's by a relative error of at most 0.00013.
Values sent between devices are 32-bit elements; how exact they have to be, the bound alone decides.
A program may use at most 128 MiB of HBM per device.

```python
import jax
import jax.numpy as jnp
from jax import lax

ITERS = 3
ZONES = 8
NX = 1024
NY = 256
NZ = 128


def with_ends(array, own_key, low, top_value):
    shape = array.shape
    spot = [jax.random.randint(jax.random.fold_in(own_key, axis), (), 0, shape[axis]) for axis in range(len(shape))]
    array = array.at[tuple(spot)].set(low)
    longest = shape.index(max(shape))
    spot[longest] = (spot[longest] + 1) % shape[longest]
    return array.at[tuple(spot)].set(top_value)


def block_scale(stream_key, shape, split, least, top_value):
    level = 1.0
    for axis_at, parts in split:
        draws = jax.random.uniform(jax.random.fold_in(jax.random.fold_in(stream_key, 6), axis_at), (parts,), jnp.float32, least / len(split), top_value / len(split))
        level = level * jnp.repeat(jnp.exp(draws), shape[axis_at] // parts).reshape((-1,) + (1,) * (len(shape) - 1 - axis_at))
    return level


def normal_values(stream_key, dims, spread, bound, pieces=(), held_as=jnp.bfloat16):
    entries = jax.random.normal(stream_key, dims, jnp.float32) * spread
    if len(pieces) > 0:
        entries = block_scale(stream_key, dims, pieces, -0.22, 0.18) * entries
    return jnp.clip(entries, min=-bound, max=bound).astype(held_as)


def setup_inputs(seed: int = 0) -> dict:
    splits = jax.random.split(jax.random.key(seed), 8)
    return {
        "density": normal_values(splits[0], (NX, NY, NZ), 1.0, 6.0, ((0, 16), (1, 8)), jnp.float32),
        "slowness": normal_values(splits[1], (NX, NY, NZ), 1.0, 6.0, ((0, 16), (1, 8)), jnp.float32),
        "pressure_obs": normal_values(splits[2], (NX, NY, NZ), 1.0, 6.0, ((0, 16), (1, 8)), jnp.float32),
        "time_obs": normal_values(splits[3], (NX, NY, NZ), 1.0, 6.0, ((0, 16), (1, 8)), jnp.float32),
        "zone_map": with_ends(jax.random.randint(splits[4], (NX, NY, NZ), 0, ZONES), jax.random.fold_in(splits[4], 1), 0, ZONES - 1).astype(jnp.int32),
        "zone_low": jnp.clip(jax.random.uniform(splits[5], (ZONES,), jnp.float32, -2.5, -0.5), -2.5, -0.5),
        "zone_high": jnp.clip(jax.random.uniform(splits[6], (ZONES,), jnp.float32, 0.5, 2.5), 0.5, 2.5),
    }


BETA = 1.0
ETA = 0.5
EPSILON = 1e-06

def slopes(field):
    padded = jnp.pad(field, 1)
    along_x = (padded[2:, 1:-1, 1:-1] - padded[:-2, 1:-1, 1:-1]) * 0.5
    along_y = (padded[1:-1, 2:, 1:-1] - padded[1:-1, :-2, 1:-1]) * 0.5
    along_z = (padded[1:-1, 1:-1, 2:] - padded[1:-1, 1:-1, :-2]) * 0.5
    return (along_x, along_y, along_z)

def slopes_adjoint(values):
    first = jnp.pad(values[0], 1)
    second = jnp.pad(values[1], 1)
    third = jnp.pad(values[2], 1)
    total = (first[:-2, 1:-1, 1:-1] - first[2:, 1:-1, 1:-1]) * 0.5
    total = total + (second[1:-1, :-2, 1:-1] - second[1:-1, 2:, 1:-1]) * 0.5
    total = total + (third[1:-1, 1:-1, :-2] - third[1:-1, 1:-1, 2:]) * 0.5
    return total

def cross_product(first_vec, second_vec):
    return (first_vec[1] * second_vec[2] - first_vec[2] * second_vec[1], first_vec[2] * second_vec[0] - first_vec[0] * second_vec[2], first_vec[0] * second_vec[1] - first_vec[1] * second_vec[0])

def reverse_cumsum(values, axis_number):
    return jnp.flip(jnp.cumsum(jnp.flip(values, axis_number), axis_number), axis_number)

def reference(density, slowness, pressure_obs, time_obs, zone_map, zone_low, zone_high):
    lower_bound = zone_low[zone_map]
    upper_bound = zone_high[zone_map]
    cells = float(NX * NY * NZ)
    zscale = 1.0 / float(NZ) ** 0.5
    xscale = 1.0 / float(NX) ** 0.5
    density_now = density
    slowness_now = slowness
    history = []
    for iteration in range(ITERS):
        first_vec = slopes(density_now)
        second_vec = slopes(slowness_now)
        crossed = cross_product(first_vec, second_vec)
        pressure_miss = jnp.cumsum(density_now, axis=2) * zscale - pressure_obs
        time_miss = jnp.cumsum(slowness_now, axis=0) * xscale - time_obs
        crossed_sq = jnp.sum(crossed[0] * crossed[0]) + jnp.sum(crossed[1] * crossed[1]) + jnp.sum(crossed[2] * crossed[2])
        history.append(0.5 * (jnp.sum(pressure_miss * pressure_miss) + jnp.sum(time_miss * time_miss) + BETA * crossed_sq) / cells)
        toward_density = cross_product(second_vec, crossed)
        toward_slowness = cross_product(crossed, first_vec)
        grad_density = reverse_cumsum(pressure_miss, 2) * zscale + BETA * slopes_adjoint(toward_density)
        grad_slowness = reverse_cumsum(time_miss, 0) * xscale + BETA * slopes_adjoint(toward_slowness)
        norm_density = jnp.sum(grad_density * grad_density)
        norm_slowness = jnp.sum(grad_slowness * grad_slowness)
        moved = density_now - ETA * grad_density * lax.rsqrt(norm_density / cells + EPSILON)
        density_now = jnp.minimum(jnp.maximum(moved, lower_bound), upper_bound)
        slowness_now = slowness_now - ETA * grad_slowness * lax.rsqrt(norm_slowness / cells + EPSILON)
    return (density_now, slowness_now, jnp.stack(history))
```

```python
import functools
import math

import jax
import jax.numpy as jnp
from jax import lax
from jax.experimental import pallas as pl
from jax.experimental.pallas import tpu as pltpu
from jax.sharding import PartitionSpec as P

ITERS = 3
ETA = 0.5
EPSILON = 1e-06
MESH = pl.DeviceIdType.MESH
PAD = 8
RIM = 2


def depth_difference(values):
    lane = lax.broadcasted_iota(jnp.int32, values.shape, values.ndim - 1)
    last = values.shape[-1] - 1
    after = pltpu.roll(values, last, values.ndim - 1)
    before = pltpu.roll(values, 1, values.ndim - 1)
    return jnp.where(lane == last, 0.0, after) - jnp.where(lane == 0, 0.0, before)


def halves(values):
    high = values.astype(jnp.bfloat16)
    low = (values - high.astype(jnp.float32)).astype(jnp.bfloat16)
    return jnp.concatenate([high, low], axis=-1)


def kernel(
    nx,
    ny,
    density,
    slowness,
    pressure,
    times,
    zones,
    low_table,
    high_table,
    density_out,
    slowness_out,
    objective,
    field,
    grads,
    zone,
    lower,
    upper,
    lever,
    fixed,
    linear,
    pobs,
    tobs,
    table,
    rev_table,
    column_send,
    column_recv,
    norm_send,
    norm_recv,
    load_sem,
    rim_send,
    rim_recv,
    zone_send,
    zone_recv,
    col_send_sem,
    col_recv_sem,
    norm_send_sem,
    norm_recv_sem,
    out_sem,
):
    sx, sy, depth = density.shape
    px, py = sx + 2 * RIM, sy + 2 * PAD
    cells = float(nx * sx * ny * sy * depth)
    zscale = 1.0 / math.sqrt(depth)
    xscale = 1.0 / math.sqrt(nx * sx)
    gx, gy = lax.axis_index("gx"), lax.axis_index("gy")
    own_x, own_y = pl.ds(RIM, sx), pl.ds(PAD, sy)

    loads = [
        pltpu.make_async_copy(slowness, field.at[1, own_x, own_y], load_sem.at[0]),
        pltpu.make_async_copy(times, tobs, load_sem.at[1]),
        pltpu.make_async_copy(density, field.at[0, own_x, own_y], load_sem.at[2]),
        pltpu.make_async_copy(zones, zone.at[own_x, own_y], load_sem.at[3]),
        pltpu.make_async_copy(pressure, pobs, load_sem.at[4]),
    ]
    for copy in loads:
        copy.start()

    def turned(value, step, size):
        return lax.rem(value + step, size)

    barrier = pltpu.get_barrier_semaphore()
    greet = [(turned(gx, k, nx), gy) for k in range(1, nx)]
    greet += [(gx, turned(gy, k, ny)) for k in range(1, ny)]
    greet += [(turned(gx, i, nx), turned(gy, j, ny)) for i in (1, nx - 1) for j in (1, ny - 1)]
    for device in greet:
        pl.semaphore_signal(barrier, inc=1, device_id=device, device_id_type=MESH)

    @pl.when(gy == 0)
    def _():
        for buffer in (field, grads):
            buffer[:, :, 0:PAD] = jnp.zeros((buffer.shape[0], px, PAD, depth), jnp.float32)

    @pl.when(gy == ny - 1)
    def _():
        for buffer in (field, grads):
            buffer[:, :, PAD + sy :] = jnp.zeros((buffer.shape[0], px, PAD, depth), jnp.float32)

    @pl.when(gx == 0)
    def _():
        for buffer in (field, grads):
            buffer[:, 0:RIM] = jnp.zeros((buffer.shape[0], RIM, py, depth), jnp.float32)

    @pl.when(gx == nx - 1)
    def _():
        for buffer in (field, grads):
            buffer[:, RIM + sx :] = jnp.zeros((buffer.shape[0], RIM, py, depth), jnp.float32)

    row = lax.broadcasted_iota(jnp.int32, (depth, depth), 0)
    col = lax.broadcasted_iota(jnp.int32, (depth, depth), 1)
    upward = jnp.where(row <= col, 1.0, 0.0).astype(jnp.bfloat16)
    both = (depth - jnp.maximum(row, col)).astype(jnp.float32).astype(jnp.bfloat16)
    downward = jnp.where(row >= col, 1.0, 0.0).astype(jnp.bfloat16)
    for half in range(2):
        rows = pl.ds(half * depth, depth)
        table[rows, pl.ds(0, depth)] = upward
        table[rows, pl.ds(depth, depth)] = both
        rev_table[rows, :] = downward

    pl.semaphore_wait(barrier, len(greet))

    def rim_copies(buffer, lead, send_sems, recv_sems):
        first_x, last_x = pl.ds(RIM, RIM), pl.ds(RIM + sx - RIM, RIM)
        before_x, after_x = pl.ds(0, RIM), pl.ds(RIM + sx, RIM)
        first_y, last_y = pl.ds(PAD, RIM), pl.ds(PAD + sy - RIM, RIM)
        before_y, after_y = pl.ds(PAD - RIM, RIM), pl.ds(PAD + sy, RIM)
        one = lambda at: pl.ds(at, 1)
        up_x, down_x, up_y, down_y = gx < nx - 1, gx > 0, gy < ny - 1, gy > 0
        plans = [
            (up_y, down_y, (0, 1), (own_x, last_y), (own_x, before_y)),
            (down_y, up_y, (0, -1), (own_x, first_y), (own_x, after_y)),
            (up_x, down_x, (1, 0), (last_x, own_y), (before_x, own_y)),
            (down_x, up_x, (-1, 0), (first_x, own_y), (after_x, own_y)),
        ]
        ends_x = {1: (one(RIM + sx - 1), one(RIM - 1)), -1: (one(RIM), one(RIM + sx))}
        ends_y = {1: (one(PAD + sy - 1), one(PAD - 1)), -1: (one(PAD), one(PAD + sy))}
        has_x = {1: (up_x, down_x), -1: (down_x, up_x)}
        has_y = {1: (up_y, down_y), -1: (down_y, up_y)}
        for i in (1, -1):
            for j in (1, -1):
                plans.append(
                    (
                        has_x[i][0] & has_y[j][0],
                        has_x[i][1] & has_y[j][1],
                        (i, j),
                        (ends_x[i][0], ends_y[j][0]),
                        (ends_x[i][1], ends_y[j][1]),
                    )
                )
        copies = []
        for k, (sends, receives, (i, j), source, target) in enumerate(plans):
            copy = pltpu.make_async_remote_copy(
                src_ref=buffer.at[(*lead, *source)],
                dst_ref=buffer.at[(*lead, *target)],
                send_sem=send_sems(k),
                recv_sem=recv_sems(k),
                device_id=(gx + i, gy + j),
                device_id_type=MESH,
            )
            copies.append((sends, receives, copy))
        return copies

    def start_rims(copies):
        for sends, _, copy in copies:
            pl.when(sends)(copy.start)

    def arrived(copies):
        for _, receives, copy in copies:
            pl.when(receives)(copy.wait_recv)

    def sent(copies):
        for sends, _, copy in copies:
            pl.when(sends)(copy.wait_send)

    def start_columns(phase):
        for k in range(1, nx):
            to = turned(gx, k, nx)
            pltpu.make_async_remote_copy(
                src_ref=column_send.at[phase, jnp.where(to > gx, 0, 1)],
                dst_ref=column_recv.at[phase, gx],
                send_sem=col_send_sem.at[phase],
                recv_sem=col_recv_sem.at[phase],
                device_id=(to, gy),
                device_id_type=MESH,
            ).start()

    def columns_arrived(phase):
        rest = column_recv.at[phase, pl.ds(0, nx - 1)]
        pltpu.make_async_copy(rest, rest, col_recv_sem.at[phase]).wait()

    def columns_summed(phase):
        zero = jnp.zeros((sy, depth), jnp.float32)
        earlier, later = zero, zero
        for k in range(nx):
            value = column_recv[phase, k]
            earlier = earlier + jnp.where(gx > k, value, 0.0)
            later = later + jnp.where(gx < k, value, 0.0)
        return earlier, later

    near = [0, 1, 2, 1]
    lane = lax.broadcasted_iota(jnp.int32, (1, depth), 1)
    steps = [(i, j) for i in range(nx) for j in range(ny) if i or j]
    if nx == 16 and ny == 8:
        steps.sort(key=lambda t: -(near[t[0] // 4] + near[t[0] % 4] + near[t[1] // 2]))
    others = nx * ny - 1

    def start_norms(phase, values):
        line = jnp.zeros((1, depth), jnp.float32)
        for k, value in enumerate(values):
            total = jnp.sum(jnp.sum(value, axis=0, keepdims=True), axis=1, keepdims=True)
            line = jnp.where(lane == k, total, line)
        norm_send[phase] = line
        to_x = [turned(gx, i, nx) for i in range(nx)]
        to_y = [turned(gy, j, ny) for j in range(ny)]
        for i, j in steps:
            pltpu.make_async_remote_copy(
                src_ref=norm_send.at[phase],
                dst_ref=norm_recv.at[phase, i * ny + j - 1],
                send_sem=norm_send_sem.at[phase],
                recv_sem=norm_recv_sem.at[phase],
                device_id=(to_x[i], to_y[j]),
                device_id_type=MESH,
            ).start()

    def norms(phase):
        everyone = norm_recv.at[phase]
        pltpu.make_async_copy(everyone, everyone, norm_recv_sem.at[phase]).wait()
        line = jnp.sum(norm_recv[phase], axis=0) + norm_send[phase]
        pick = lambda k: jnp.sum(jnp.where(lane == k, line, 0.0), axis=1, keepdims=True)
        step_density = ETA * lax.rsqrt(pick(0) * (1.0 / cells) + EPSILON)
        step_slowness = ETA * lax.rsqrt(pick(1) * (1.0 / cells) + EPSILON)
        objective[phase] = jnp.sum(jnp.where(lane == 2, line, 0.0)) * (0.5 / cells)
        return step_density, step_slowness

    loads[0].wait()
    loads[1].wait()

    def first_sums(x, carry):
        running, weighted, observed = carry
        running = running + field[1, x + RIM, own_y]
        return running, weighted + running, observed + tobs[x]

    zero = jnp.zeros((sy, depth), jnp.float32)
    total, weighted, observed = lax.fori_loop(0, sx, first_sums, (zero, zero, zero), unroll=4)
    later_parts = (nx - 1 - gx).astype(jnp.float32) * float(sx)
    column_send[0, 0] = total
    column_send[0, 1] = xscale * (weighted + later_parts * total) - observed
    loads[2].wait()
    rims = rim_copies(
        field, (pl.ds(0, 2),), lambda k: rim_send.at[0, k], lambda k: rim_recv.at[0, k]
    )
    start_rims(rims)
    start_columns(0)
    loads[3].wait()
    zone_rims = rim_copies(zone, (), lambda k: zone_send.at[k], lambda k: zone_recv.at[k])
    start_rims(zone_rims)

    loads[4].wait()
    planes = 8

    def fix(step, carry):
        at = pl.multiple_of(step * planes, planes)
        values = pobs[pl.ds(at, planes)].reshape(planes * sy, depth)
        back = jnp.dot(halves(values), rev_table[...], preferred_element_type=jnp.float32)
        fixed[pl.ds(at, planes)] = (back * zscale).reshape(planes, sy, depth)
        return carry

    lax.fori_loop(0, sx // planes, fix, 0)

    def integrate(values, at, squares):
        out = jnp.dot(
            halves(values.reshape(planes * sy, depth)),
            table[...],
            preferred_element_type=jnp.float32,
        )
        miss = out[:, :depth] * zscale - pobs[pl.ds(at, planes)].reshape(planes * sy, depth)
        pull = (out[:, depth:] * (zscale * zscale)).reshape(planes, sy, depth)
        linear[pl.ds(at, planes)] = pull - fixed[pl.ds(at, planes)]
        return squares + jnp.sum((miss * miss).reshape(planes * sy // 8, 8, depth), axis=0)

    zero_tile = jnp.zeros((8, depth), jnp.float32)

    def first_integrals(step, squares):
        at = pl.multiple_of(step * planes, planes)
        return integrate(field[0, pl.ds(at + RIM, planes), own_y], at, squares)

    miss_squares = lax.fori_loop(0, sx // planes, first_integrals, zero_tile)

    def look_up(x, carry):
        number = zone[x]
        low = jnp.zeros(number.shape, jnp.float32)
        high = low
        for k in range(low_table.shape[0]):
            hit = number == k
            low = jnp.where(hit, low_table[k], low)
            high = jnp.where(hit, high_table[k], high)
        lower[x] = low
        upper[x] = high
        return carry

    wide = pl.ds(PAD - 1, sy + 8)

    def levers(p, squares):
        first_vec, second_vec = [], []
        for index, vec in ((0, first_vec), (1, second_vec)):
            vec.append(field[index, p + 1, wide] - field[index, p - 1, wide])
            vec.append(field[index, p, pl.ds(PAD, sy + 8)] - field[index, p, pl.ds(PAD - 2, sy + 8)])
            vec.append(depth_difference(field[index, p, wide]))
        crossed = cross(first_vec, second_vec)
        for index, value in enumerate(cross(second_vec, crossed)):
            lever[index, p, wide] = value
        for index, value in enumerate(cross(crossed, first_vec)):
            lever[3 + index, p, wide] = value
        return squares + (
            crossed[0] * crossed[0] + crossed[1] * crossed[1] + crossed[2] * crossed[2]
        )

    def cross(u, v):
        return (u[1] * v[2] - u[2] * v[1], u[2] * v[0] - u[0] * v[2], u[0] * v[1] - u[1] * v[0])

    def spread(index, p):
        along_x = lever[index, p - 1, own_y] - lever[index, p + 1, own_y]
        along_y = lever[index + 1, p, pl.ds(PAD - 1, sy)] - lever[index + 1, p, pl.ds(PAD + 1, sy)]
        return along_x + along_y - depth_difference(lever[index + 2, p, own_y])

    before = after = None
    rim_sets = [rims]
    for phase in range(ITERS):
        if phase == 0:
            arrived(rims)
        zero_wide = jnp.zeros((sy + 8, depth), jnp.float32)
        crossed_squares = lax.fori_loop(
            RIM, RIM + sx, levers, zero_wide, unroll=2
        )
        levers(RIM - 1, zero_wide)
        levers(RIM + sx, zero_wide)
        wide_row = lax.broadcasted_iota(jnp.int32, zero_wide.shape, 0)
        crossed_squares = jnp.where(
            (wide_row >= 1) & (wide_row < sy + 1), crossed_squares, 0.0
        )
        crossed_squares = jnp.sum(crossed_squares.reshape(-1, 8, depth), axis=0)

        columns_arrived(phase)
        earlier, later = columns_summed(phase)
        if phase == 0:
            before = earlier
            after = (
                later
                + (xscale * later_parts) * (before + total)
                + xscale * (weighted + float(sx) * before)
                - observed
            )
        else:
            after = after - step_slowness * xscale * (
                later
                + later_parts * (earlier + total)
                + weighted
                + float(sx) * earlier
            )
            before = before - step_slowness * earlier

        if phase > 1:
            sent(rim_sets[phase - 1])
        slot = phase % 2

        def descend(x, carry):
            running, ahead, total, weighted, time_squares, squares_d, squares_s = carry
            p = x + RIM
            pull = linear[x] + spread(0, p) * (1.0 / 16.0)
            grads[2 * slot, p, own_y] = pull
            running = running + xscale * field[1, p, own_y]
            miss = running - tobs[x]
            push = xscale * ahead + spread(3, p) * (1.0 / 16.0)
            ahead = ahead - miss
            grads[2 * slot + 1, p, own_y] = push
            total = total + push
            weighted = weighted + total
            return (
                running,
                ahead,
                total,
                weighted,
                time_squares + miss * miss,
                squares_d + pull * pull,
                squares_s + push * push,
            )

        carry = (xscale * before, after, zero, zero, zero, zero, zero)
        _, _, total, weighted, time_squares, squares_d, squares_s = lax.fori_loop(
            0, sx, descend, carry, unroll=2
        )
        tile = lambda v: jnp.sum(v.reshape(sy // 8, 8, depth), axis=0)
        start_norms(
            phase,
            (
                tile(squares_d),
                tile(squares_s),
                tile(time_squares) + miss_squares + crossed_squares * (1.0 / 16.0),
            ),
        )
        if phase < ITERS - 1:
            new_rims = rim_copies(
                grads,
                (pl.ds(2 * slot, 2),),
                lambda k, phase=phase: rim_send.at[phase + 1, k],
                lambda k, phase=phase: rim_recv.at[phase + 1, k],
            )
            rim_sets.append(new_rims)
            start_rims(new_rims)
            column_send[phase + 1, 0] = total
            column_send[phase + 1, 1] = weighted + later_parts * total
            start_columns(phase + 1)
        if phase == 0:
            sent(rims)
            arrived(zone_rims)
            sent(zone_rims)
            lax.fori_loop(0, px, look_up, 0)
        step_density, step_slowness = norms(phase)
        if phase < ITERS - 1:
            arrived(new_rims)

            def move_rim(p, rows):
                d = field[0, p, rows] - step_density * grads[2 * slot, p, rows]
                field[0, p, rows] = jnp.minimum(jnp.maximum(d, lower[p, rows]), upper[p, rows])
                field[1, p, rows] = field[1, p, rows] - step_slowness * grads[2 * slot + 1, p, rows]

            for p in (*range(RIM), *range(RIM + sx, px)):
                move_rim(p, pl.ds(0, py))

            def move(step, squares):
                at = pl.multiple_of(step * planes, planes)
                span = pl.ds(at + RIM, planes)
                d = field[0, span, own_y] - step_density * grads[2 * slot, span, own_y]
                d = jnp.minimum(jnp.maximum(d, lower[span, own_y]), upper[span, own_y])
                field[0, span, own_y] = d
                field[1, span, own_y] = (
                    field[1, span, own_y] - step_slowness * grads[2 * slot + 1, span, own_y]
                )
                for k in range(planes):
                    move_rim(at + RIM + k, pl.ds(0, PAD))
                    move_rim(at + RIM + k, pl.ds(PAD + sy, PAD))
                return integrate(d, at, squares)

            miss_squares = lax.fori_loop(0, sx // planes, move, zero_tile)
        else:

            def finish(x, carry):
                p = x + RIM
                d = field[0, p, own_y] - step_density * grads[2 * slot, p, own_y]
                density_out[x] = jnp.minimum(jnp.maximum(d, lower[p, own_y]), upper[p, own_y])
                slowness_out[x] = field[1, p, own_y] - step_slowness * grads[2 * slot + 1, p, own_y]
                return carry

            lax.fori_loop(0, sx, finish, 0, unroll=2)

    sent(rim_sets[-1])
    for phase in range(ITERS):
        rest = column_recv.at[phase, pl.ds(0, nx - 1)]
        pltpu.make_async_copy(rest, rest, col_send_sem.at[phase]).wait()
        everyone = norm_recv.at[phase]
        pltpu.make_async_copy(everyone, everyone, norm_send_sem.at[phase]).wait()


def solution(mesh):
    nx, ny = mesh.shape["gx"], mesh.shape["gy"]

    def local(density, slowness, pressure, times, zones, low_table, high_table):
        sx, sy, depth = density.shape
        px, py = sx + 2 * RIM, sy + 2 * PAD
        f32, bf16 = jnp.float32, jnp.bfloat16
        hbm = pl.BlockSpec(memory_space=pl.ANY)
        smem = pl.BlockSpec(memory_space=pltpu.SMEM)
        vmem = pl.BlockSpec(memory_space=pltpu.VMEM)
        dma = pltpu.SemaphoreType.DMA
        model = jax.ShapeDtypeStruct((sx, sy, depth), f32)
        return pl.pallas_call(
            functools.partial(kernel, nx, ny),
            out_shape=(model, model, jax.ShapeDtypeStruct((ITERS,), f32)),
            in_specs=[hbm] * 5 + [smem] * 2,
            out_specs=(vmem, vmem, smem),
            scratch_shapes=[
                pltpu.VMEM((2, px, py, depth), f32),
                pltpu.VMEM((4, px, py, depth), f32),
                pltpu.VMEM((px, py, depth), jnp.int32),
                pltpu.VMEM((px, py, depth), f32),
                pltpu.VMEM((px, py, depth), f32),
                pltpu.VMEM((6, px, py, depth), f32),
                pltpu.VMEM((sx, sy, depth), f32),
                pltpu.VMEM((sx, sy, depth), f32),
                pltpu.VMEM((sx, sy, depth), f32),
                pltpu.VMEM((sx, sy, depth), f32),
                pltpu.VMEM((2 * depth, 2 * depth), bf16),
                pltpu.VMEM((2 * depth, depth), bf16),
                pltpu.VMEM((ITERS, 2, sy, depth), f32),
                pltpu.VMEM((ITERS, nx, sy, depth), f32),
                pltpu.VMEM((ITERS, 1, depth), f32),
                pltpu.VMEM((ITERS, nx * ny - 1, 1, depth), f32),
                dma((5,)),
                dma((ITERS, 8)),
                dma((ITERS, 8)),
                dma((8,)),
                dma((8,)),
                dma((ITERS,)),
                dma((ITERS,)),
                dma((ITERS,)),
                dma((ITERS,)),
                dma((2,)),
            ],
            compiler_params=pltpu.CompilerParams(
                collective_id=0,
                has_side_effects=True,
                vmem_limit_bytes=52 * 1024 * 1024,
            ),
        )(density, slowness, pressure, times, zones, low_table, high_table)

    part = P("gx", "gy", None)
    return jax.shard_map(
        local,
        mesh=mesh,
        in_specs=(part,) * 5 + (P(), P()),
        out_specs=(part, part, P()),
        check_vma=False,
    )
```

```python
import functools
import math

import jax
import jax.numpy as jnp
from jax import lax
from jax.experimental import pallas as pl
from jax.experimental.pallas import tpu as pltpu
from jax.sharding import PartitionSpec as P

ITERS = 3
ETA = 0.5
EPSILON = 1e-06
MESH = pl.DeviceIdType.MESH
PAD = 8
RIM = 2
WHOLE = 16.0
BATCH = 4


def depth_difference(values):
    lane = lax.broadcasted_iota(jnp.int32, values.shape, values.ndim - 1)
    last = values.shape[-1] - 1
    after = pltpu.roll(values, last, values.ndim - 1)
    before = pltpu.roll(values, 1, values.ndim - 1)
    return jnp.where(lane == last, 0.0, after) - jnp.where(lane == 0, 0.0, before)


def halves(values):
    high = values.astype(jnp.bfloat16)
    low = (values - high.astype(jnp.float32)).astype(jnp.bfloat16)
    return jnp.concatenate([high, low], axis=-1)


def kernel(
    nx,
    ny,
    density,
    slowness,
    pressure,
    times,
    zones,
    lows,
    highs,
    density_out,
    slowness_out,
    objective,
    field,
    grads,
    zone,
    lower,
    upper,
    lever,
    twist,
    slope,
    turn,
    cums,
    pulls,
    fixed,
    pobs,
    tobs,
    lhs,
    table,
    rev_table,
    low_table,
    high_table,
    column_send,
    column_recv,
    norm_send,
    norm_recv,
    load_sem,
    rim_send,
    rim_recv,
    zone_send,
    zone_recv,
    col_send_sem,
    col_recv_sem,
    norm_send_sem,
    norm_recv_sem,
    state,
):
    sx, sy, depth = density.shape
    px, py = sx + 2 * RIM, sy + 2 * PAD
    cells = float(nx * sx * ny * sy * depth)
    zscale = 1.0 / math.sqrt(depth)
    xscale = 1.0 / math.sqrt(nx * sx)
    gx, gy = lax.axis_index("gx"), lax.axis_index("gy")
    own_x, own_y = pl.ds(RIM, sx), pl.ds(PAD, sy)

    loads = [
        pltpu.make_async_copy(slowness, field.at[1, own_x, own_y], load_sem.at[0]),
        pltpu.make_async_copy(times, tobs, load_sem.at[1]),
        pltpu.make_async_copy(density, field.at[0, own_x, own_y], load_sem.at[2]),
        pltpu.make_async_copy(zones, zone.at[own_x, own_y], load_sem.at[3]),
        pltpu.make_async_copy(pressure, pobs, load_sem.at[4]),
        pltpu.make_async_copy(lows, low_table, load_sem.at[5]),
        pltpu.make_async_copy(highs, high_table, load_sem.at[6]),
    ]
    for copy in loads:
        copy.start()

    def turned(value, step, size):
        return lax.rem(value + step, size)

    barrier = pltpu.get_barrier_semaphore()
    greet = [(turned(gx, k, nx), gy) for k in range(1, nx)]
    greet += [(gx, turned(gy, k, ny)) for k in range(1, ny)]
    greet += [(turned(gx, i, nx), turned(gy, j, ny)) for i in (1, nx - 1) for j in (1, ny - 1)]
    for device in greet:
        pl.semaphore_signal(barrier, inc=1, device_id=device, device_id_type=MESH)

    @pl.when(gy == 0)
    def _():
        for buffer in (field, grads):
            buffer[:, :, 0:PAD] = jnp.zeros((buffer.shape[0], px, PAD, depth), jnp.float32)

    @pl.when(gy == ny - 1)
    def _():
        for buffer in (field, grads):
            buffer[:, :, PAD + sy :] = jnp.zeros((buffer.shape[0], px, PAD, depth), jnp.float32)

    @pl.when(gx == 0)
    def _():
        for buffer in (field, grads):
            buffer[:, 0:RIM] = jnp.zeros((buffer.shape[0], RIM, py, depth), jnp.float32)

    @pl.when(gx == nx - 1)
    def _():
        for buffer in (field, grads):
            buffer[:, RIM + sx :] = jnp.zeros((buffer.shape[0], RIM, py, depth), jnp.float32)

    row = lax.broadcasted_iota(jnp.int32, (depth, depth), 0)
    col = lax.broadcasted_iota(jnp.int32, (depth, depth), 1)
    upward = jnp.where(row <= col, 1.0, 0.0).astype(jnp.bfloat16)
    both = ((depth - jnp.maximum(row, col)).astype(jnp.float32) * (WHOLE / depth)).astype(jnp.bfloat16)
    differ = (jnp.where(row == col + 1, 1.0, 0.0) - jnp.where(row == col - 1, 1.0, 0.0)).astype(jnp.bfloat16)
    downward = jnp.where(row >= col, 1.0, 0.0).astype(jnp.bfloat16)
    for half in range(2):
        tall = pl.ds(half * depth, depth)
        table[tall, pl.ds(0, depth)] = upward
        table[tall, pl.ds(depth, depth)] = both
        table[tall, pl.ds(2 * depth, depth)] = differ
        rev_table[tall, :] = downward

    pl.semaphore_wait(barrier, len(greet))

    def rim_copies(buffer, lead, send_sems, recv_sems):
        first_x, last_x = pl.ds(RIM, RIM), pl.ds(RIM + sx - RIM, RIM)
        before_x, after_x = pl.ds(0, RIM), pl.ds(RIM + sx, RIM)
        first_y, last_y = pl.ds(PAD, RIM), pl.ds(PAD + sy - RIM, RIM)
        before_y, after_y = pl.ds(PAD - RIM, RIM), pl.ds(PAD + sy, RIM)
        one = lambda at: pl.ds(at, 1)
        up_x, down_x, up_y, down_y = gx < nx - 1, gx > 0, gy < ny - 1, gy > 0
        plans = [
            (up_y, down_y, (0, 1), (own_x, last_y), (own_x, before_y)),
            (down_y, up_y, (0, -1), (own_x, first_y), (own_x, after_y)),
            (up_x, down_x, (1, 0), (last_x, own_y), (before_x, own_y)),
            (down_x, up_x, (-1, 0), (first_x, own_y), (after_x, own_y)),
        ]
        ends_x = {1: (one(RIM + sx - 1), one(RIM - 1)), -1: (one(RIM), one(RIM + sx))}
        ends_y = {1: (one(PAD + sy - 1), one(PAD - 1)), -1: (one(PAD), one(PAD + sy))}
        has_x = {1: (up_x, down_x), -1: (down_x, up_x)}
        has_y = {1: (up_y, down_y), -1: (down_y, up_y)}
        for i in (1, -1):
            for j in (1, -1):
                plans.append(
                    (
                        has_x[i][0] & has_y[j][0],
                        has_x[i][1] & has_y[j][1],
                        (i, j),
                        (ends_x[i][0], ends_y[j][0]),
                        (ends_x[i][1], ends_y[j][1]),
                    )
                )
        copies = []
        for k, (sends, receives, (i, j), source, target) in enumerate(plans):
            copy = pltpu.make_async_remote_copy(
                src_ref=buffer.at[(*lead, *source)],
                dst_ref=buffer.at[(*lead, *target)],
                send_sem=send_sems(k),
                recv_sem=recv_sems(k),
                device_id=(gx + i, gy + j),
                device_id_type=MESH,
            )
            copies.append((sends, receives, copy))
        return copies

    def start_rims(copies):
        for sends, _, copy in copies:
            pl.when(sends)(copy.start)

    def arrived(copies):
        for _, receives, copy in copies:
            pl.when(receives)(copy.wait_recv)

    def sent(copies):
        for sends, _, copy in copies:
            pl.when(sends)(copy.wait_send)

    def start_columns(phase):
        for k in range(1, nx):
            to = turned(gx, k, nx)
            pltpu.make_async_remote_copy(
                src_ref=column_send.at[phase, jnp.where(to > gx, 0, 1)],
                dst_ref=column_recv.at[phase, gx],
                send_sem=col_send_sem.at[phase],
                recv_sem=col_recv_sem.at[phase],
                device_id=(to, gy),
                device_id_type=MESH,
            ).start()

    def columns_arrived(phase):
        rest = column_recv.at[phase, pl.ds(0, nx - 1)]
        pltpu.make_async_copy(rest, rest, col_recv_sem.at[phase]).wait()

    def columns_summed(phase):
        zero = jnp.zeros((sy, depth), jnp.float32)
        earlier, later = zero, zero
        for k in range(nx):
            value = column_recv[phase, k]
            earlier = earlier + jnp.where(gx > k, value, 0.0)
            later = later + jnp.where(gx < k, value, 0.0)
        return earlier, later

    near = [0, 1, 2, 1]
    lane = lax.broadcasted_iota(jnp.int32, (1, depth), 1)
    steps = [(i, j) for i in range(nx) for j in range(ny) if i or j]
    if nx == 16 and ny == 8:
        steps.sort(key=lambda t: -(near[t[0] // 4] + near[t[0] % 4] + near[t[1] // 2]))
    others = nx * ny - 1

    def start_norms(phase, values):
        line = jnp.zeros((1, depth), jnp.float32)
        for k, value in enumerate(values):
            total = jnp.sum(jnp.sum(value, axis=0, keepdims=True), axis=1, keepdims=True)
            line = jnp.where(lane == k, total, line)
        norm_send[phase] = line
        to_x = [turned(gx, i, nx) for i in range(nx)]
        to_y = [turned(gy, j, ny) for j in range(ny)]
        for i, j in steps:
            pltpu.make_async_remote_copy(
                src_ref=norm_send.at[phase],
                dst_ref=norm_recv.at[phase, i * ny + j - 1],
                send_sem=norm_send_sem.at[phase],
                recv_sem=norm_recv_sem.at[phase],
                device_id=(to_x[i], to_y[j]),
                device_id_type=MESH,
            ).start()

    def norms(phase):
        everyone = norm_recv.at[phase]
        pltpu.make_async_copy(everyone, everyone, norm_recv_sem.at[phase]).wait()
        line = jnp.sum(norm_recv[phase], axis=0) + norm_send[phase]
        pick = lambda k: jnp.sum(jnp.where(lane == k, line, 0.0), axis=1, keepdims=True)
        scale = 1.0 / (WHOLE * WHOLE * cells)
        step_density = (ETA / WHOLE) * lax.rsqrt(pick(0) * scale + EPSILON)
        step_slowness = (ETA / WHOLE) * lax.rsqrt(pick(1) * scale + EPSILON)
        objective[phase] = jnp.sum(jnp.where(lane == 2, line, 0.0)) * (0.5 / cells)
        return step_density, step_slowness

    loads[0].wait()
    loads[1].wait()

    def first_sums(x, carry):
        running, weighted, observed = carry
        running = running + field[1, x + RIM, own_y]
        seen = tobs[x]
        tobs[x] = seen * (1.0 / xscale)
        return running, weighted + running, observed + seen

    zero = jnp.zeros((sy, depth), jnp.float32)
    loads[2].wait()
    rims = rim_copies(
        field, (pl.ds(0, 2),), lambda k: rim_send.at[0, k], lambda k: rim_recv.at[0, k]
    )
    start_rims(rims)
    total, weighted, observed = lax.fori_loop(0, sx, first_sums, (zero, zero, zero), unroll=4)
    later_parts = (nx - 1 - gx).astype(jnp.float32) * float(sx)
    column_send[0, 0] = total
    column_send[0, 1] = xscale * (weighted + later_parts * total) - observed
    start_columns(0)
    loads[3].wait()
    zone_rims = rim_copies(zone, (), lambda k: zone_send.at[k], lambda k: zone_recv.at[k])
    start_rims(zone_rims)

    loads[4].wait()
    planes = 8
    tall = planes * sy

    def fix(step, carry):
        span = pl.ds(pl.multiple_of(step * planes, planes), planes)
        values = pobs[span].reshape(tall, depth)
        back = jnp.dot(halves(values), rev_table[...], preferred_element_type=jnp.float32)
        fixed[span] = (back * (WHOLE * zscale)).reshape(planes, sy, depth)
        pobs[span] = (values * (1.0 / zscale)).reshape(planes, sy, depth)
        return carry

    lax.fori_loop(0, sx // planes, fix, 0, unroll=2)

    def integrate(step):
        span = pl.ds(pl.multiple_of(step * planes, planes), planes)
        flat = pl.ds(pl.multiple_of(step * tall, tall), tall)
        out = jnp.dot(lhs[flat], table[...], preferred_element_type=jnp.float32)
        for buffer, k in ((cums, 0), (pulls, 1), (slope.at[0], 2)):
            buffer[span] = out[:, k * depth : (k + 1) * depth].reshape(planes, sy, depth)

    def in_steps(prepare):
        prepare(0)

        def body(step, carry):
            integrate(step - 1)
            prepare(step)
            return carry

        lax.fori_loop(1, sx // planes, body, 0)
        integrate(sx // planes - 1)

    def fill(step, values):
        lhs[pl.ds(pl.multiple_of(step * tall, tall), tall)] = halves(values.reshape(tall, depth))

    in_steps(lambda k: fill(k, field[0, pl.ds(pl.multiple_of(k * planes, planes) + RIM, planes), own_y]))

    def all_slopes(source, target):
        def body(step, carry):
            at = pl.multiple_of(step * planes, planes)
            target[pl.ds(at, planes)] = depth_difference(source[pl.ds(at + RIM, planes), own_y])
            return carry

        lax.fori_loop(0, sx // planes, body, 0)

    all_slopes(field.at[1], slope.at[1])

    def look_up(x, carry):
        number = zone[x]
        low = jnp.zeros(number.shape, jnp.float32)
        high = low
        for k in range(low_table.shape[0]):
            hit = number == k
            low = jnp.where(hit, low_table[k], low)
            high = jnp.where(hit, high_table[k], high)
        lower[x] = low
        upper[x] = high
        return carry

    groups = sy // 8
    zero_tile = jnp.zeros((8, depth), jnp.float32)
    none = (zero_tile,) * groups

    def rows(j):
        return pl.ds(PAD + j, 8, stride=groups)

    def own(j):
        return pl.ds(j, 8, stride=groups)

    def tree(values):
        values = list(values)
        while len(values) > 1:
            values = [sum(values[k : k + 2]) for k in range(0, len(values), 2)]
        return values[0]

    ring = pl.ds(PAD - 1, 2, stride=sy + 1)
    ring_after = pl.ds(PAD, 2, stride=sy + 1)
    ring_before = pl.ds(PAD - 2, 2, stride=sy + 1)

    def edge_levers(p):
        for j in range(groups):
            first_vec, second_vec = [
                (
                    field[f, p + 1, rows(j)] - field[f, p - 1, rows(j)],
                    field[f, p, rows(j + 1)] - field[f, p, rows(j - 1)],
                    depth_difference(field[f, p, rows(j)]),
                )
                for f in range(2)
            ]
            crossed = cross(first_vec, second_vec)
            lever[0, p, rows(j)] = cross(second_vec, crossed)[0]
            lever[2, p, rows(j)] = cross(crossed, first_vec)[0]

    def plane_levers(x):
        p = x + RIM
        center = [[field[f, p, rows(j)] for j in range(-1, groups + 1)] for f in range(2)]
        squares = []
        for j in range(groups):
            first_vec, second_vec = [
                (
                    field[f, p + 1, rows(j)] - field[f, p - 1, rows(j)],
                    center[f][j + 2] - center[f][j],
                    slope[f, x, own(j)],
                )
                for f in range(2)
            ]
            crossed = cross(first_vec, second_vec)
            for f, vec in ((0, cross(second_vec, crossed)), (1, cross(crossed, first_vec))):
                lever[2 * f, p, rows(j)] = vec[0]
                lever[2 * f + 1, p, rows(j)] = vec[1]
                twist[f, x + BATCH, own(j)] = vec[2]
            squares.append(tree([c * c for c in crossed]))
        first_vec, second_vec = [
            (
                field[f, p + 1, ring] - field[f, p - 1, ring],
                field[f, p, ring_after] - field[f, p, ring_before],
                depth_difference(field[f, p, ring]),
            )
            for f in range(2)
        ]
        crossed = cross(first_vec, second_vec)
        lever[1, p, ring] = cross(second_vec, crossed)[1]
        lever[3, p, ring] = cross(crossed, first_vec)[1]
        return tree(squares)

    def untwist(at):
        for f in range(2):
            for k in range(BATCH):
                for j in range(groups):
                    twist[f, at + k, own(j)] = depth_difference(twist[f, at + k, own(j)])

    def levers(step, squares):
        x = step * BATCH
        untwist(x)
        return squares + tree([plane_levers(x + k) for k in range(BATCH)])

    def cross(u, v):
        return (u[1] * v[2] - u[2] * v[1], u[2] * v[0] - u[0] * v[2], u[0] * v[1] - u[1] * v[0])

    def spread(f, x):
        p = x + RIM
        along = [lever[2 * f + 1, p, rows(j)] for j in range(-1, groups + 1)]
        return [
            (lever[2 * f, p - 1, rows(j)] - lever[2 * f, p + 1, rows(j)])
            + ((along[j] - along[j + 2]) - twist[f, x + BATCH, own(j)])
            for j in range(groups)
        ]

    before = ahead = None
    rim_sets = [rims]
    for phase in range(ITERS):
        if phase == 0:
            arrived(rims)
        none = (zero_tile,) * groups
        crossed_squares = lax.fori_loop(0, sx // BATCH, levers, zero_tile)
        untwist(sx)
        edge_levers(RIM - 1)
        edge_levers(RIM + sx)

        columns_arrived(phase)
        earlier, later = columns_summed(phase)
        if phase == 0:
            before = earlier
            ahead = (
                later * (1.0 / xscale)
                + later_parts * (before + total)
                + (weighted + float(sx) * before)
                - observed * (1.0 / xscale)
            )
        else:
            ahead = ahead - step_slowness * (
                later + later_parts * (earlier + total) + weighted + float(sx) * earlier
            )
            before = before - step_slowness * earlier

        if phase > 1:
            sent(rim_sets[phase - 1])
        slot = phase % 2

        push_scale = WHOLE * xscale * xscale

        def descend(step, carry):
            running, push_sum, total, weighted, squares = map(list, carry)
            for k in range(BATCH):
                x = step * BATCH + k
                p = x + RIM
                spreads = spread(0, x), spread(1, x)
                terms = [[], [], [], []]
                for j in range(groups):
                    fit = cums[x, own(j)] - pobs[x, own(j)]
                    pull = (pulls[x, own(j)] - fixed[x, own(j)]) + spreads[0][j]
                    grads[2 * slot, p, rows(j)] = pull
                    running[j] = running[j] + field[1, p, rows(j)]
                    miss = running[j] - tobs[x, own(j)]
                    push = push_scale * push_sum[j] + spreads[1][j]
                    push_sum[j] = push_sum[j] - miss
                    grads[2 * slot + 1, p, rows(j)] = push
                    total[j] = total[j] + push
                    weighted[j] = weighted[j] + total[j]
                    for term, value in zip(terms, (pull, push, fit, miss)):
                        term.append(value * value)
                squares = [square + tree(term) for square, term in zip(squares, terms)]
            return tuple(map(tuple, (running, push_sum, total, weighted, squares)))

        state[0] = before
        state[1] = ahead
        split = lambda k: tuple(state[k, own(j)] for j in range(groups))
        carry = (split(0), split(1), none, none, (zero_tile,) * 4)
        _, _, totals, weights, squares = lax.fori_loop(0, sx // BATCH, descend, carry)
        for j in range(groups):
            state[0, own(j)] = totals[j]
            state[1, own(j)] = weights[j]
        total, weighted = state[0], state[1]
        start_norms(
            phase,
            (
                squares[0],
                squares[1],
                squares[2] * (zscale * zscale)
                + squares[3] * (xscale * xscale)
                + crossed_squares * (1.0 / 16.0),
            ),
        )
        if phase < ITERS - 1:
            new_rims = rim_copies(
                grads,
                (pl.ds(2 * slot, 2),),
                lambda k, phase=phase: rim_send.at[phase + 1, k],
                lambda k, phase=phase: rim_recv.at[phase + 1, k],
            )
            rim_sets.append(new_rims)
            start_rims(new_rims)
            column_send[phase + 1, 0] = total
            column_send[phase + 1, 1] = weighted + later_parts * total
            start_columns(phase + 1)
        if phase == 0:
            sent(rims)
            arrived(zone_rims)
            sent(zone_rims)
            loads[5].wait()
            loads[6].wait()
            lax.fori_loop(0, px, look_up, 0)
        if phase < ITERS - 1:
            all_slopes(grads.at[2 * slot + 1], turn)
        step_density, step_slowness = norms(phase)
        if phase < ITERS - 1:
            arrived(new_rims)

            def move_rim(p, at):
                d = field[0, p, at] - step_density * grads[2 * slot, p, at]
                field[0, p, at] = jnp.minimum(jnp.maximum(d, lower[p, at]), upper[p, at])
                field[1, p, at] = field[1, p, at] - step_slowness * grads[2 * slot + 1, p, at]

            for p in (*range(RIM), *range(RIM + sx, px)):
                move_rim(p, pl.ds(0, py))

            def move(step):
                at = pl.multiple_of(step * planes, planes)
                span = pl.ds(at + RIM, planes)
                d = field[0, span, own_y] - step_density * grads[2 * slot, span, own_y]
                d = jnp.minimum(jnp.maximum(d, lower[span, own_y]), upper[span, own_y])
                field[0, span, own_y] = d
                fill(step, d)
                field[1, span, own_y] = (
                    field[1, span, own_y] - step_slowness * grads[2 * slot + 1, span, own_y]
                )
                slope[1, pl.ds(at, planes)] = (
                    slope[1, pl.ds(at, planes)] - step_slowness * turn[pl.ds(at, planes)]
                )
                for k in range(planes):
                    move_rim(at + RIM + k, pl.ds(0, PAD))
                    move_rim(at + RIM + k, pl.ds(PAD + sy, PAD))

            in_steps(move)
        else:

            def finish(x, carry):
                p = x + RIM
                d = field[0, p, own_y] - step_density * grads[2 * slot, p, own_y]
                density_out[x] = jnp.minimum(jnp.maximum(d, lower[p, own_y]), upper[p, own_y])
                slowness_out[x] = field[1, p, own_y] - step_slowness * grads[2 * slot + 1, p, own_y]
                return carry

            lax.fori_loop(0, sx, finish, 0, unroll=2)

    sent(rim_sets[-1])
    for phase in range(ITERS):
        rest = column_recv.at[phase, pl.ds(0, nx - 1)]
        pltpu.make_async_copy(rest, rest, col_send_sem.at[phase]).wait()
        everyone = norm_recv.at[phase]
        pltpu.make_async_copy(everyone, everyone, norm_send_sem.at[phase]).wait()


def solution(mesh):
    nx, ny = mesh.shape["gx"], mesh.shape["gy"]

    def local(density, slowness, pressure, times, zones, low_table, high_table):
        sx, sy, depth = density.shape
        zones_shape = low_table.shape
        px, py = sx + 2 * RIM, sy + 2 * PAD
        f32, bf16 = jnp.float32, jnp.bfloat16
        hbm = pl.BlockSpec(memory_space=pltpu.HBM)
        smem = pl.BlockSpec(memory_space=pltpu.SMEM)
        vmem = pl.BlockSpec(memory_space=pltpu.VMEM)
        dma = pltpu.SemaphoreType.DMA
        model = jax.ShapeDtypeStruct((sx, sy, depth), f32)
        return pl.pallas_call(
            functools.partial(kernel, nx, ny),
            out_shape=(model, model, jax.ShapeDtypeStruct((ITERS,), f32)),
            in_specs=[hbm] * 7,
            out_specs=(vmem, vmem, smem),
            scratch_shapes=[
                pltpu.VMEM((2, px, py, depth), f32),
                pltpu.VMEM((4, px, py, depth), f32),
                pltpu.VMEM((px, py, depth), jnp.int32),
                pltpu.VMEM((px, py, depth), f32),
                pltpu.VMEM((px, py, depth), f32),
                pltpu.VMEM((4, px, py, depth), f32),
                pltpu.VMEM((2, sx + BATCH, sy, depth), f32),
                pltpu.VMEM((2, sx, sy, depth), f32),
                *[pltpu.VMEM((sx, sy, depth), f32)] * 6,
                pltpu.VMEM((sx * sy, 2 * depth), bf16),
                pltpu.VMEM((2 * depth, 3 * depth), bf16),
                pltpu.VMEM((2 * depth, depth), bf16),
                pltpu.SMEM(zones_shape, f32),
                pltpu.SMEM(zones_shape, f32),
                pltpu.VMEM((ITERS, 2, sy, depth), f32),
                pltpu.VMEM((ITERS, nx, sy, depth), f32),
                pltpu.VMEM((ITERS, 1, depth), f32),
                pltpu.VMEM((ITERS, nx * ny - 1, 1, depth), f32),
                dma((7,)),
                dma((ITERS, 8)),
                dma((ITERS, 8)),
                dma((8,)),
                dma((8,)),
                dma((ITERS,)),
                dma((ITERS,)),
                dma((ITERS,)),
                dma((ITERS,)),
                pltpu.VMEM((2, sy, depth), f32),
            ],
            compiler_params=pltpu.CompilerParams(
                collective_id=0,
                has_side_effects=True,
                vmem_limit_bytes=54 * 1024 * 1024,
            ),
        )(density, slowness, pressure, times, zones, low_table, high_table)

    part = P("gx", "gy", None)
    return jax.shard_map(
        local,
        mesh=mesh,
        in_specs=(part,) * 5 + (P(), P()),
        out_specs=(part, part, P()),
        check_vma=False,
    )
```

```python
import functools
import math

import jax
import jax.numpy as jnp
from jax import lax
from jax.experimental import pallas as pl
from jax.experimental.pallas import tpu as pltpu
from jax.sharding import PartitionSpec as P

ITERS = 3
ETA = 0.5
EPSILON = 1e-06
MESH = pl.DeviceIdType.MESH
PAD = 8
RIM = 2
LONG = 32
WHOLE = 16.0
BATCH = 4


def depth_difference(values):
    lane = lax.broadcasted_iota(jnp.int32, values.shape, values.ndim - 1)
    last = values.shape[-1] - 1
    after = pltpu.roll(values, last, values.ndim - 1)
    before = pltpu.roll(values, 1, values.ndim - 1)
    return jnp.where(lane == last, 0.0, after) - jnp.where(lane == 0, 0.0, before)


def halves(values):
    high = values.astype(jnp.bfloat16)
    low = (values - high.astype(jnp.float32)).astype(jnp.bfloat16)
    return jnp.concatenate([high, low], axis=-1)


def steps_of(line, cells):
    lane = lax.broadcasted_iota(jnp.int32, line.shape, 1)
    scale = 1.0 / (WHOLE * WHOLE * cells)
    norm = lambda k: jnp.sum(jnp.where(lane == k, line, 0.0), axis=1, keepdims=True) * scale
    return [(ETA / WHOLE) * lax.rsqrt(norm(k) + EPSILON) for k in range(2)]


def finish(
    cells,
    density,
    pull,
    lower,
    upper,
    slowness,
    push,
    lines,
    density_out,
    slowness_out,
    objective,
    density_new,
    slowness_new,
    sem,
):
    step_density, step_slowness = steps_of(lines[ITERS - 1], cells)
    pieces = 4
    length = density.shape[0] // pieces
    copies = []
    for k in range(pieces):
        span = pl.ds(k * length, length)

        def body(x, carry):
            moved = density[x] - step_density * pull[x]
            density_new[x] = jnp.minimum(jnp.maximum(moved, lower[x]), upper[x])
            slowness_new[x] = slowness[x] - step_slowness * push[x]
            return carry

        lax.fori_loop(k * length, (k + 1) * length, body, 0, unroll=2)
        for source, target in ((density_new, density_out), (slowness_new, slowness_out)):
            copies.append(
                pltpu.make_async_copy(source.at[span], target.at[span], sem.at[len(copies)])
            )
            copies[-1].start()
    lane = lax.broadcasted_iota(jnp.int32, (1, lines.shape[-1]), 1)
    pick = lambda phase, k: jnp.where(lane == k, lines[phase], 0.0)
    for phase in range(ITERS):
        parts = pick(phase, 2)
        if phase < ITERS - 1:
            parts = parts + pick(phase + 1, 3)
        objective[phase] = jnp.sum(parts) * (0.5 / cells)
    for copy in copies:
        copy.wait()


def kernel(
    nx,
    ny,
    density,
    slowness,
    pressure,
    times,
    zones,
    lows,
    highs,
    density_out,
    pull_out,
    lower_out,
    upper_out,
    slowness_out,
    push_out,
    lines_out,
    field,
    grads,
    zone,
    lower,
    upper,
    lever,
    twist,
    twist_lhs,
    slope,
    turn,
    pulls,
    fixed,
    pobs,
    tobs,
    lhs,
    table,
    rev_table,
    up_table,
    low_table,
    high_table,
    column_send,
    column_recv,
    norm_send,
    norm_recv,
    load_sem,
    rim_send,
    rim_recv,
    zone_send,
    zone_recv,
    col_send_sem,
    col_recv_sem,
    norm_send_sem,
    norm_recv_sem,
    state,
):
    sx, sy, depth = density.shape
    px, py = sx + 2 * RIM, sy + 2 * PAD
    cells = float(nx * sx * ny * sy * depth)
    zscale = 1.0 / math.sqrt(depth)
    xscale = 1.0 / math.sqrt(nx * sx)
    gx, gy = lax.axis_index("gx"), lax.axis_index("gy")
    own_x, own_y = pl.ds(RIM, sx), pl.ds(PAD, sy)

    loads = [
        pltpu.make_async_copy(slowness, field.at[1, own_x, own_y], load_sem.at[0]),
        pltpu.make_async_copy(times, tobs, load_sem.at[1]),
        pltpu.make_async_copy(density, field.at[0, own_x, own_y], load_sem.at[2]),
        pltpu.make_async_copy(zones, zone.at[own_x, own_y], load_sem.at[3]),
        pltpu.make_async_copy(pressure, pobs, load_sem.at[4]),
        pltpu.make_async_copy(lows, low_table, load_sem.at[5]),
        pltpu.make_async_copy(highs, high_table, load_sem.at[6]),
    ]
    for copy in loads:
        copy.start()

    def turned(value, step, size):
        return lax.rem(value + step, size)

    barrier = pltpu.get_barrier_semaphore()
    greet = [(turned(gx, k, nx), gy) for k in range(1, nx)]
    greet += [(gx, turned(gy, k, ny)) for k in range(1, ny)]
    greet += [(turned(gx, i, nx), turned(gy, j, ny)) for i in (1, nx - 1) for j in (1, ny - 1)]
    for device in greet:
        pl.semaphore_signal(barrier, inc=1, device_id=device, device_id_type=MESH)

    @pl.when(gy == 0)
    def _():
        for buffer in (field, grads):
            buffer[:, :, 0:PAD] = jnp.zeros((buffer.shape[0], px, PAD, depth), jnp.float32)

    @pl.when(gy == ny - 1)
    def _():
        for buffer in (field, grads):
            buffer[:, :, PAD + sy :] = jnp.zeros((buffer.shape[0], px, PAD, depth), jnp.float32)

    @pl.when(gx == 0)
    def _():
        for buffer in (field, grads):
            buffer[:, 0:RIM] = jnp.zeros((buffer.shape[0], RIM, py, depth), jnp.float32)

    @pl.when(gx == nx - 1)
    def _():
        for buffer in (field, grads):
            buffer[:, RIM + sx :] = jnp.zeros((buffer.shape[0], RIM, py, depth), jnp.float32)

    row = lax.broadcasted_iota(jnp.int32, (depth, depth), 0)
    col = lax.broadcasted_iota(jnp.int32, (depth, depth), 1)
    upward = jnp.where(row <= col, 1.0, 0.0).astype(jnp.bfloat16)
    both = ((depth - jnp.maximum(row, col)).astype(jnp.float32) * (WHOLE / depth)).astype(jnp.bfloat16)
    differ = (jnp.where(row == col + 1, 1.0, 0.0) - jnp.where(row == col - 1, 1.0, 0.0)).astype(jnp.bfloat16)
    downward = jnp.where(row >= col, 1.0, 0.0).astype(jnp.bfloat16)
    for half in range(2):
        tall = pl.ds(half * depth, depth)
        table[tall, pl.ds(0, depth)] = both
        table[tall, pl.ds(depth, depth)] = differ
        up_table[tall, :] = upward
        rev_table[tall, :] = downward

    pl.semaphore_wait(barrier, len(greet))

    def rim_copies(buffer, lead, send_sems, recv_sems):
        first_x, last_x = pl.ds(RIM, RIM), pl.ds(RIM + sx - RIM, RIM)
        before_x, after_x = pl.ds(0, RIM), pl.ds(RIM + sx, RIM)
        first_y, last_y = pl.ds(PAD, RIM), pl.ds(PAD + sy - RIM, RIM)
        before_y, after_y = pl.ds(PAD - RIM, RIM), pl.ds(PAD + sy, RIM)
        one = lambda at: pl.ds(at, 1)
        up_x, down_x, up_y, down_y = gx < nx - 1, gx > 0, gy < ny - 1, gy > 0
        plans = [
            (up_y, down_y, (0, 1), (own_x, last_y), (own_x, before_y)),
            (down_y, up_y, (0, -1), (own_x, first_y), (own_x, after_y)),
            (up_x, down_x, (1, 0), (last_x, own_y), (before_x, own_y)),
            (down_x, up_x, (-1, 0), (first_x, own_y), (after_x, own_y)),
        ]
        ends_x = {1: (one(RIM + sx - 1), one(RIM - 1)), -1: (one(RIM), one(RIM + sx))}
        ends_y = {1: (one(PAD + sy - 1), one(PAD - 1)), -1: (one(PAD), one(PAD + sy))}
        has_x = {1: (up_x, down_x), -1: (down_x, up_x)}
        has_y = {1: (up_y, down_y), -1: (down_y, up_y)}
        for i in (1, -1):
            for j in (1, -1):
                plans.append(
                    (
                        has_x[i][0] & has_y[j][0],
                        has_x[i][1] & has_y[j][1],
                        (i, j),
                        (ends_x[i][0], ends_y[j][0]),
                        (ends_x[i][1], ends_y[j][1]),
                    )
                )
        copies = []
        for k, (sends, receives, (i, j), source, target) in enumerate(plans):
            copy = pltpu.make_async_remote_copy(
                src_ref=buffer.at[(*lead, *source)],
                dst_ref=buffer.at[(*lead, *target)],
                send_sem=send_sems(k),
                recv_sem=recv_sems(k),
                device_id=(gx + i, gy + j),
                device_id_type=MESH,
            )
            copies.append((sends, receives, copy))
        return copies

    def start_rims(copies):
        for sends, _, copy in copies:
            pl.when(sends)(copy.start)

    def arrived(copies):
        for _, receives, copy in copies:
            pl.when(receives)(copy.wait_recv)

    def sent(copies):
        for sends, _, copy in copies:
            pl.when(sends)(copy.wait_send)

    def start_columns(phase):
        for k in range(1, nx):
            to = turned(gx, k, nx)
            pltpu.make_async_remote_copy(
                src_ref=column_send.at[phase, jnp.where(to > gx, 0, 1)],
                dst_ref=column_recv.at[phase, gx],
                send_sem=col_send_sem.at[phase],
                recv_sem=col_recv_sem.at[phase],
                device_id=(to, gy),
                device_id_type=MESH,
            ).start()

    def columns_arrived(phase):
        rest = column_recv.at[phase, pl.ds(0, nx - 1)]
        pltpu.make_async_copy(rest, rest, col_recv_sem.at[phase]).wait()

    def columns_summed(phase):
        zero = jnp.zeros((sy, depth), jnp.float32)
        earlier, later = zero, zero
        for k in range(nx):
            value = column_recv[phase, k]
            earlier = earlier + jnp.where(gx > k, value, 0.0)
            later = later + jnp.where(gx < k, value, 0.0)
        return earlier, later

    near = [0, 1, 2, 1]
    lane = lax.broadcasted_iota(jnp.int32, (1, depth), 1)
    steps = [(i, j) for i in range(nx) for j in range(ny) if i or j]
    if nx == 16 and ny == 8:
        steps.sort(key=lambda t: -(near[t[0] // 4] + near[t[0] % 4] + near[t[1] // 2]))
    others = nx * ny - 1

    def start_norms(phase, values):
        line = jnp.zeros((1, depth), jnp.float32)
        for k, value in enumerate(values):
            total = jnp.sum(jnp.sum(value, axis=0, keepdims=True), axis=1, keepdims=True)
            line = jnp.where(lane == k, total, line)
        norm_send[phase] = line
        to_x = [turned(gx, i, nx) for i in range(nx)]
        to_y = [turned(gy, j, ny) for j in range(ny)]
        for i, j in steps:
            pltpu.make_async_remote_copy(
                src_ref=norm_send.at[phase],
                dst_ref=norm_recv.at[phase, i * ny + j - 1],
                send_sem=norm_send_sem.at[phase],
                recv_sem=norm_recv_sem.at[phase],
                device_id=(to_x[i], to_y[j]),
                device_id_type=MESH,
            ).start()

    def norms(phase):
        everyone = norm_recv.at[phase]
        pltpu.make_async_copy(everyone, everyone, norm_recv_sem.at[phase]).wait()
        line = jnp.sum(norm_recv[phase], axis=0) + norm_send[phase]
        lines_out[phase] = line
        return steps_of(line, cells)

    loads[0].wait()
    loads[1].wait()

    def first_sums(x, carry):
        running, weighted, observed = carry
        running = running + field[1, x + RIM, own_y]
        seen = tobs[x]
        tobs[x] = seen * (1.0 / xscale)
        return running, weighted + running, observed + seen

    zero = jnp.zeros((sy, depth), jnp.float32)
    loads[2].wait()
    rims = rim_copies(
        field, (pl.ds(0, 2),), lambda k: rim_send.at[0, k], lambda k: rim_recv.at[0, k]
    )
    start_rims(rims)
    total, weighted, observed = lax.fori_loop(0, sx, first_sums, (zero, zero, zero), unroll=4)
    later_parts = (nx - 1 - gx).astype(jnp.float32) * float(sx)
    column_send[0, 0] = total
    column_send[0, 1] = xscale * (weighted + later_parts * total) - observed
    start_columns(0)

    loads[4].wait()
    planes = 8
    tall = planes * sy

    def fix(step, carry):
        span = pl.ds(pl.multiple_of(step * planes, planes), planes)
        values = pobs[span].reshape(tall, depth)
        back = jnp.dot(halves(values), rev_table[...], preferred_element_type=jnp.float32)
        fixed[span] = (back * (WHOLE * zscale)).reshape(planes, sy, depth)
        pobs[span] = (values * (1.0 / zscale)).reshape(planes, sy, depth)
        return carry

    lax.fori_loop(0, sx // planes, fix, 0, unroll=2)

    long = min(LONG, sx)

    def integrate():
        for step in range(sx // long):
            span = pl.ds(step * long, long)
            out = jnp.dot(
                lhs[pl.ds(step * long * sy, long * sy)],
                table[...],
                preferred_element_type=jnp.float32,
            )
            pulls[span] = out[:, :depth].reshape(long, sy, depth)
            slope[0, span] = out[:, depth:].reshape(long, sy, depth)

    def fits():
        def body(step, squares):
            out = jnp.dot(
                lhs[pl.ds(pl.multiple_of(step * long * sy, 8), long * sy)],
                up_table[...],
                preferred_element_type=jnp.float32,
            )
            miss = out - pobs[pl.ds(step * long, long)].reshape(long * sy, depth)
            return squares + jnp.sum((miss * miss).reshape(long * sy // 8, 8, depth), axis=0)

        return lax.fori_loop(0, sx // long, body, zero_tile)

    def fill(step, values):
        lhs[pl.ds(pl.multiple_of(step * tall, tall), tall)] = halves(values.reshape(tall, depth))

    def first_fill(k, carry):
        fill(k, field[0, pl.ds(pl.multiple_of(k * planes, planes) + RIM, planes), own_y])
        return carry

    lax.fori_loop(0, sx // planes, first_fill, 0)
    integrate()

    def all_slopes(source, target):
        def body(step, carry):
            at = pl.multiple_of(step * planes, planes)
            target[pl.ds(at, planes)] = depth_difference(source[pl.ds(at + RIM, planes), own_y])
            return carry

        lax.fori_loop(0, sx // planes, body, 0)

    all_slopes(field.at[1], slope.at[1])

    def look_up(x, carry):
        number = zone[x]
        low = jnp.zeros(number.shape, jnp.float32)
        high = low
        for k in range(low_table.shape[0]):
            hit = number == k
            low = jnp.where(hit, low_table[k], low)
            high = jnp.where(hit, high_table[k], high)
        lower[x] = low
        upper[x] = high
        return carry

    groups = sy // 8
    zero_tile = jnp.zeros((8, depth), jnp.float32)
    none = (zero_tile,) * groups

    def rows(j):
        return pl.ds(PAD + j, 8, stride=groups)

    def own(j):
        return pl.ds(j, 8, stride=groups)

    def tree(values):
        values = list(values)
        while len(values) > 1:
            values = [sum(values[k : k + 2]) for k in range(0, len(values), 2)]
        return values[0]

    ring = pl.ds(PAD - 1, 2, stride=sy + 1)
    ring_after = pl.ds(PAD, 2, stride=sy + 1)
    ring_before = pl.ds(PAD - 2, 2, stride=sy + 1)

    def edge_levers(p):
        for j in range(groups):
            first_vec, second_vec = [
                (
                    field[f, p + 1, rows(j)] - field[f, p - 1, rows(j)],
                    field[f, p, rows(j + 1)] - field[f, p, rows(j - 1)],
                    depth_difference(field[f, p, rows(j)]),
                )
                for f in range(2)
            ]
            crossed = cross(first_vec, second_vec)
            lever[0, p, rows(j)] = cross(second_vec, crossed)[0]
            lever[2, p, rows(j)] = cross(crossed, first_vec)[0]

    def plane_levers(x):
        p = x + RIM
        center = [[field[f, p, rows(j)] for j in range(-1, groups + 1)] for f in range(2)]
        squares = []
        twists = [], []
        for j in range(groups):
            first_vec, second_vec = [
                (
                    field[f, p + 1, rows(j)] - field[f, p - 1, rows(j)],
                    center[f][j + 2] - center[f][j],
                    slope[f, x, own(j)],
                )
                for f in range(2)
            ]
            crossed = cross(first_vec, second_vec)
            for f, vec in ((0, cross(second_vec, crossed)), (1, cross(crossed, first_vec))):
                lever[2 * f, p, rows(j)] = vec[0]
                lever[2 * f + 1, p, rows(j)] = vec[1]
                twists[f].append(vec[2])
            squares.append(tree([c * c for c in crossed]))
        for f in range(2):
            for j in range(0, groups, 2):
                twist_lhs[f, pl.ds(pl.multiple_of(x * sy, 16) + 8 * j, 16)] = halves(
                    jnp.concatenate(twists[f][j : j + 2], axis=0)
                )
        first_vec, second_vec = [
            (
                field[f, p + 1, ring] - field[f, p - 1, ring],
                field[f, p, ring_after] - field[f, p, ring_before],
                depth_difference(field[f, p, ring]),
            )
            for f in range(2)
        ]
        crossed = cross(first_vec, second_vec)
        lever[1, p, ring] = cross(second_vec, crossed)[1]
        lever[3, p, ring] = cross(crossed, first_vec)[1]
        return tree(squares)

    def untwist():
        for f in range(2):
            for step in range(sx // long):
                out = jnp.dot(
                    twist_lhs[f, pl.ds(step * long * sy, long * sy)],
                    table[:, pl.ds(depth, depth)],
                    preferred_element_type=jnp.float32,
                )
                twist[f, pl.ds(step * long, long)] = out.reshape(long, sy, depth)

    def levers(step, squares):
        x = step * BATCH
        return squares + tree([plane_levers(x + k) for k in range(BATCH)])

    def cross(u, v):
        return (u[1] * v[2] - u[2] * v[1], u[2] * v[0] - u[0] * v[2], u[0] * v[1] - u[1] * v[0])

    def spread(f, x):
        p = x + RIM
        along = [lever[2 * f + 1, p, rows(j)] for j in range(-1, groups + 1)]
        return [
            (lever[2 * f, p - 1, rows(j)] - lever[2 * f, p + 1, rows(j)])
            + ((along[j] - along[j + 2]) - twist[f, x, pl.ds(8 * j, 8)])
            for j in range(groups)
        ]

    before = ahead = None
    fit_squares = late_squares = zero_tile
    rim_sets = [rims]
    for phase in range(ITERS):
        if phase == 0:
            arrived(rims)
        none = (zero_tile,) * groups
        crossed_squares = lax.fori_loop(0, sx // BATCH, levers, zero_tile)
        edge_levers(RIM - 1)
        edge_levers(RIM + sx)
        untwist()

        if phase == 0:
            loads[3].wait()
            zone_rims = rim_copies(zone, (), lambda k: zone_send.at[k], lambda k: zone_recv.at[k])
            start_rims(zone_rims)
        columns_arrived(phase)
        earlier, later = columns_summed(phase)
        if phase == 0:
            before = earlier
            ahead = (
                later * (1.0 / xscale)
                + later_parts * (before + total)
                + (weighted + float(sx) * before)
                - observed * (1.0 / xscale)
            )
        else:
            ahead = ahead - step_slowness * (
                later + later_parts * (earlier + total) + weighted + float(sx) * earlier
            )
            before = before - step_slowness * earlier

        if phase > 1:
            sent(rim_sets[phase - 1])
        slot = phase % 2

        if phase == ITERS - 1:
            late_squares = fits()
        push_scale = WHOLE * xscale * xscale

        def descend(step, carry):
            running, push_sum, total, weighted, squares = map(list, carry)
            for k in range(BATCH):
                x = step * BATCH + k
                p = x + RIM
                spreads = spread(0, x), spread(1, x)
                terms = [[], [], []]
                for j in range(groups):
                    pull = (pulls[x, own(j)] - fixed[x, own(j)]) + spreads[0][j]
                    if phase < ITERS - 1:
                        grads[2 * slot, p, rows(j)] = pull
                    else:
                        pull_out[x, own(j)] = pull
                    running[j] = running[j] + field[1, p, rows(j)]
                    miss = running[j] - tobs[x, own(j)]
                    push = push_scale * push_sum[j] + spreads[1][j]
                    push_sum[j] = push_sum[j] - miss
                    if phase < ITERS - 1:
                        grads[2 * slot + 1, p, rows(j)] = push
                    else:
                        push_out[x, own(j)] = push
                    total[j] = total[j] + push
                    weighted[j] = weighted[j] + total[j]
                    for term, value in zip(terms, (pull, push, miss)):
                        term.append(value * value)
                squares = [square + tree(term) for square, term in zip(squares, terms)]
            return tuple(map(tuple, (running, push_sum, total, weighted, squares)))

        state[0] = before
        state[1] = ahead
        split = lambda k: tuple(state[k, own(j)] for j in range(groups))
        carry = (split(0), split(1), none, none, (zero_tile,) * 3)
        _, _, totals, weights, squares = lax.fori_loop(0, sx // BATCH, descend, carry)
        for j in range(groups):
            state[0, own(j)] = totals[j]
            state[1, own(j)] = weights[j]
        total, weighted = state[0], state[1]
        start_norms(
            phase,
            (
                squares[0],
                squares[1],
                squares[2] * (xscale * xscale)
                + crossed_squares * (1.0 / 16.0)
                + late_squares * (zscale * zscale),
                fit_squares * (zscale * zscale),
            ),
        )
        if phase < ITERS - 1:
            new_rims = rim_copies(
                grads,
                (pl.ds(2 * slot, 2),),
                lambda k, phase=phase: rim_send.at[phase + 1, k],
                lambda k, phase=phase: rim_recv.at[phase + 1, k],
            )
            rim_sets.append(new_rims)
            start_rims(new_rims)
            column_send[phase + 1, 0] = total
            column_send[phase + 1, 1] = weighted + later_parts * total
            start_columns(phase + 1)
        if phase == 0:
            sent(rims)
            arrived(zone_rims)
            sent(zone_rims)
            loads[5].wait()
            loads[6].wait()
            lax.fori_loop(0, px, look_up, 0)
        if phase < ITERS - 1:
            all_slopes(grads.at[2 * slot + 1], turn)
            fit_squares = fits()
        else:

            def hand_over(x, carry):
                p = x + RIM
                density_out[x] = field[0, p, own_y]
                slowness_out[x] = field[1, p, own_y]
                lower_out[x] = lower[p, own_y]
                upper_out[x] = upper[p, own_y]
                return carry

            lax.fori_loop(0, sx, hand_over, 0, unroll=2)
        step_density, step_slowness = norms(phase)
        if phase < ITERS - 1:
            arrived(new_rims)

            def move_rim(p, at):
                d = field[0, p, at] - step_density * grads[2 * slot, p, at]
                field[0, p, at] = jnp.minimum(jnp.maximum(d, lower[p, at]), upper[p, at])
                field[1, p, at] = field[1, p, at] - step_slowness * grads[2 * slot + 1, p, at]

            for p in (*range(RIM), *range(RIM + sx, px)):
                move_rim(p, pl.ds(0, py))

            def move(step, carry):
                at = pl.multiple_of(step * planes, planes)
                span = pl.ds(at + RIM, planes)
                d = field[0, span, own_y] - step_density * grads[2 * slot, span, own_y]
                d = jnp.minimum(jnp.maximum(d, lower[span, own_y]), upper[span, own_y])
                field[0, span, own_y] = d
                fill(step, d)
                field[1, span, own_y] = (
                    field[1, span, own_y] - step_slowness * grads[2 * slot + 1, span, own_y]
                )
                slope[1, pl.ds(at, planes)] = (
                    slope[1, pl.ds(at, planes)] - step_slowness * turn[pl.ds(at, planes)]
                )
                for k in range(planes):
                    move_rim(at + RIM + k, pl.ds(0, PAD))
                    move_rim(at + RIM + k, pl.ds(PAD + sy, PAD))
                return carry

            lax.fori_loop(0, sx // planes, move, 0)
            integrate()
    sent(rim_sets[-1])
    for phase in range(ITERS):
        rest = column_recv.at[phase, pl.ds(0, nx - 1)]
        pltpu.make_async_copy(rest, rest, col_send_sem.at[phase]).wait()
        everyone = norm_recv.at[phase]
        pltpu.make_async_copy(everyone, everyone, norm_send_sem.at[phase]).wait()


def solution(mesh):
    nx, ny = mesh.shape["gx"], mesh.shape["gy"]

    def local(density, slowness, pressure, times, zones, low_table, high_table):
        sx, sy, depth = density.shape
        zones_shape = low_table.shape
        px, py = sx + 2 * RIM, sy + 2 * PAD
        f32, bf16 = jnp.float32, jnp.bfloat16
        hbm = pl.BlockSpec(memory_space=pltpu.HBM)
        smem = pl.BlockSpec(memory_space=pltpu.SMEM)
        vmem = pl.BlockSpec(memory_space=pltpu.VMEM)
        dma = pltpu.SemaphoreType.DMA
        model = jax.ShapeDtypeStruct((sx, sy, depth), f32)
        inputs = (density, slowness, pressure, times, zones, low_table, high_table)
        last = pl.pallas_call(
            functools.partial(kernel, nx, ny),
            out_shape=(model,) * 6 + (jax.ShapeDtypeStruct((ITERS, 1, depth), f32),),
            in_specs=[hbm] * 7,
            out_specs=(vmem,) * 7,
            scratch_shapes=[
                pltpu.VMEM((2, px, py, depth), f32),
                pltpu.VMEM((4, px, py, depth), f32),
                pltpu.VMEM((px, py, depth), jnp.int32),
                pltpu.VMEM((px, py, depth), f32),
                pltpu.VMEM((px, py, depth), f32),
                pltpu.VMEM((4, px, py, depth), f32),
                pltpu.VMEM((2, sx, sy, depth), f32),
                pltpu.VMEM((2, sx * sy, 2 * depth), bf16),
                pltpu.VMEM((2, sx, sy, depth), f32),
                *[pltpu.VMEM((sx, sy, depth), f32)] * 5,
                pltpu.VMEM((sx * sy, 2 * depth), bf16),
                pltpu.VMEM((2 * depth, 2 * depth), bf16),
                pltpu.VMEM((2 * depth, depth), bf16),
                pltpu.VMEM((2 * depth, depth), bf16),
                pltpu.SMEM(zones_shape, f32),
                pltpu.SMEM(zones_shape, f32),
                pltpu.VMEM((ITERS, 2, sy, depth), f32),
                pltpu.VMEM((ITERS, nx, sy, depth), f32),
                pltpu.VMEM((ITERS, 1, depth), f32),
                pltpu.VMEM((ITERS, nx * ny - 1, 1, depth), f32),
                dma((7,)),
                dma((ITERS, 8)),
                dma((ITERS, 8)),
                dma((8,)),
                dma((8,)),
                dma((ITERS,)),
                dma((ITERS,)),
                dma((ITERS,)),
                dma((ITERS,)),
                pltpu.VMEM((2, sy, depth), f32),
            ],
            compiler_params=pltpu.CompilerParams(
                collective_id=0,
                has_side_effects=True,
                vmem_limit_bytes=44 * 1024 * 1024,
            ),
        )(*[pltpu.with_memory_space_constraint(value, pltpu.HBM) for value in inputs])
        return pl.pallas_call(
            functools.partial(finish, float(nx * sx * ny * sy * depth)),
            out_shape=(model, model, jax.ShapeDtypeStruct((ITERS,), f32)),
            in_specs=[vmem] * 7,
            out_specs=(pl.BlockSpec(memory_space=pl.ANY),) * 2 + (smem,),
            scratch_shapes=[
                pltpu.VMEM((sx, sy, depth), f32),
                pltpu.VMEM((sx, sy, depth), f32),
                dma((8,)),
            ],
            compiler_params=pltpu.CompilerParams(vmem_limit_bytes=8 * 1024 * 1024),
        )(*last)

    part = P("gx", "gy", None)
    return jax.shard_map(
        local,
        mesh=mesh,
        in_specs=(part,) * 5 + (P(), P()),
        out_specs=(part, part, P()),
        check_vma=False,
    )
```

```python
import functools
import math

import jax
import jax.numpy as jnp
from jax import lax
from jax.experimental import pallas as pl
from jax.experimental.pallas import tpu as pltpu
from jax.sharding import PartitionSpec as P

ITERS = 3
ETA = 0.5
EPSILON = 1e-06
MESH = pl.DeviceIdType.MESH
PAD = 8
RIM = 2
LONG = 32
WHOLE = 16.0
BATCH = 8


def depth_difference(values):
    lane = lax.broadcasted_iota(jnp.int32, values.shape, values.ndim - 1)
    last = values.shape[-1] - 1
    after = pltpu.roll(values, last, values.ndim - 1)
    before = pltpu.roll(values, 1, values.ndim - 1)
    return jnp.where(lane == last, 0.0, after) - jnp.where(lane == 0, 0.0, before)


def halves(values):
    high = values.astype(jnp.bfloat16)
    low = (values - high.astype(jnp.float32)).astype(jnp.bfloat16)
    return jnp.concatenate([high, low], axis=-1)


def steps_of(line, cells):
    lane = lax.broadcasted_iota(jnp.int32, line.shape, 1)
    scale = 1.0 / (WHOLE * WHOLE * cells)
    norm = lambda k: jnp.sum(jnp.where(lane == k, line, 0.0), axis=1, keepdims=True) * scale
    return [(ETA / WHOLE) * lax.rsqrt(norm(k) + EPSILON) for k in range(2)]


def finish(
    cells,
    density,
    pull,
    lower,
    upper,
    slowness,
    push,
    lines,
    density_out,
    slowness_out,
    objective,
    density_new,
    slowness_new,
    sem,
):
    step_density, step_slowness = steps_of(lines[ITERS - 1], cells)
    pieces = 8
    length = density.shape[0] // pieces
    copies = []
    for k in range(pieces):
        span = pl.ds(k * length, length)

        def body(x, carry):
            moved = density[x] - step_density * pull[x]
            density_new[x] = jnp.minimum(jnp.maximum(moved, lower[x]), upper[x])
            slowness_new[x] = slowness[x] - step_slowness * push[x]
            return carry

        lax.fori_loop(k * length, (k + 1) * length, body, 0, unroll=2)
        for source, target in ((density_new, density_out), (slowness_new, slowness_out)):
            copies.append(
                pltpu.make_async_copy(source.at[span], target.at[span], sem.at[len(copies)])
            )
            copies[-1].start()
    lane = lax.broadcasted_iota(jnp.int32, (1, lines.shape[-1]), 1)
    pick = lambda phase, k: jnp.where(lane == k, lines[phase], 0.0)
    for phase in range(ITERS):
        parts = pick(phase, 2)
        if phase < ITERS - 1:
            parts = parts + pick(phase + 1, 3)
        objective[phase] = jnp.sum(parts) * (0.5 / cells)
    for copy in copies:
        copy.wait()


def kernel(
    nx,
    ny,
    density,
    slowness,
    pressure,
    times,
    zones,
    lows,
    highs,
    density_out,
    pull_out,
    lower_out,
    upper_out,
    slowness_out,
    push_out,
    lines_out,
    field,
    grads,
    zone,
    lower,
    upper,
    lever,
    twist,
    twist_lhs,
    slope,
    turn,
    pulls,
    fixed,
    pobs,
    tobs,
    lhs,
    table,
    rev_table,
    up_table,
    low_table,
    high_table,
    column_send,
    column_recv,
    norm_send,
    norm_recv,
    load_sem,
    rim_send,
    rim_recv,
    zone_send,
    zone_recv,
    col_send_sem,
    col_recv_sem,
    norm_send_sem,
    norm_recv_sem,
    state,
):
    sx, sy, depth = density.shape
    px, py = sx + 2 * RIM, sy + 2 * PAD
    cells = float(nx * sx * ny * sy * depth)
    zscale = 1.0 / math.sqrt(depth)
    xscale = 1.0 / math.sqrt(nx * sx)
    gx, gy = lax.axis_index("gx"), lax.axis_index("gy")
    own_x, own_y = pl.ds(RIM, sx), pl.ds(PAD, sy)

    loads = [
        pltpu.make_async_copy(slowness, field.at[1, own_x, own_y], load_sem.at[0]),
        pltpu.make_async_copy(times, tobs, load_sem.at[1]),
        pltpu.make_async_copy(density, field.at[0, own_x, own_y], load_sem.at[2]),
        pltpu.make_async_copy(zones, zone.at[own_x, own_y], load_sem.at[3]),
        pltpu.make_async_copy(pressure, pobs, load_sem.at[4]),
        pltpu.make_async_copy(lows, low_table, load_sem.at[5]),
        pltpu.make_async_copy(highs, high_table, load_sem.at[6]),
    ]
    for copy in loads:
        copy.start()

    def turned(value, step, size):
        return lax.rem(value + step, size)

    near = [0, 1, 2, 1]

    def far_first(steps):
        if (nx, ny) == (16, 8):
            steps = sorted(steps, key=lambda t: -(near[t[0] // 4] + near[t[0] % 4] + near[t[1] // 2]))
        return steps

    barrier = pltpu.get_barrier_semaphore()
    steps_x = [i for i, _ in far_first([(i, 0) for i in range(1, nx)])]
    greet = [(i, 0) for i in range(1, nx)] + [(0, j) for j in range(1, ny)]
    greet += [(i, j) for i in (1, nx - 1) for j in (1, ny - 1)]
    for i, j in far_first(greet):
        device = (turned(gx, i, nx), turned(gy, j, ny))
        pl.semaphore_signal(barrier, inc=1, device_id=device, device_id_type=MESH)

    @pl.when(gy == 0)
    def _():
        for buffer in (field, grads):
            buffer[:, :, 0:PAD] = jnp.zeros((buffer.shape[0], px, PAD, depth), jnp.float32)

    @pl.when(gy == ny - 1)
    def _():
        for buffer in (field, grads):
            buffer[:, :, PAD + sy :] = jnp.zeros((buffer.shape[0], px, PAD, depth), jnp.float32)

    @pl.when(gx == 0)
    def _():
        for buffer in (field, grads):
            buffer[:, 0:RIM] = jnp.zeros((buffer.shape[0], RIM, py, depth), jnp.float32)

    @pl.when(gx == nx - 1)
    def _():
        for buffer in (field, grads):
            buffer[:, RIM + sx :] = jnp.zeros((buffer.shape[0], RIM, py, depth), jnp.float32)

    row = lax.broadcasted_iota(jnp.int32, (depth, depth), 0)
    col = lax.broadcasted_iota(jnp.int32, (depth, depth), 1)
    upward = jnp.where(row <= col, 1.0, 0.0).astype(jnp.bfloat16)
    both = ((depth - jnp.maximum(row, col)).astype(jnp.float32) * (WHOLE / depth)).astype(jnp.bfloat16)
    differ = (jnp.where(row == col + 1, 1.0, 0.0) - jnp.where(row == col - 1, 1.0, 0.0)).astype(jnp.bfloat16)
    downward = jnp.where(row >= col, 1.0, 0.0).astype(jnp.bfloat16)
    for half in range(2):
        tall = pl.ds(half * depth, depth)
        table[tall, pl.ds(0, depth)] = both
        table[tall, pl.ds(depth, depth)] = differ
        table[tall, pl.ds(2 * depth, depth)] = upward
        up_table[tall, :] = upward
        rev_table[tall, :] = downward

    loads[0].wait()
    loads[1].wait()

    def first_sums(x, carry):
        running, weighted, observed = carry
        running = running + field[1, x + RIM, own_y]
        seen = tobs[x]
        tobs[x] = seen * (1.0 / xscale)
        return running, weighted + running, observed + seen

    zero = jnp.zeros((sy, depth), jnp.float32)
    total, weighted, observed = lax.fori_loop(0, sx, first_sums, (zero, zero, zero), unroll=4)
    later_parts = (nx - 1 - gx).astype(jnp.float32) * float(sx)
    column_send[0, 0] = total
    column_send[0, 1] = xscale * (weighted + later_parts * total) - observed
    pl.semaphore_wait(barrier, len(greet))

    def rim_copies(buffer, lead, send_sems, recv_sems):
        first_x, last_x = pl.ds(RIM, RIM), pl.ds(RIM + sx - RIM, RIM)
        before_x, after_x = pl.ds(0, RIM), pl.ds(RIM + sx, RIM)
        first_y, last_y = pl.ds(PAD, RIM), pl.ds(PAD + sy - RIM, RIM)
        before_y, after_y = pl.ds(PAD - RIM, RIM), pl.ds(PAD + sy, RIM)
        one = lambda at: pl.ds(at, 1)
        up_x, down_x, up_y, down_y = gx < nx - 1, gx > 0, gy < ny - 1, gy > 0
        plans = [
            (up_y, down_y, (0, 1), (own_x, last_y), (own_x, before_y)),
            (down_y, up_y, (0, -1), (own_x, first_y), (own_x, after_y)),
            (up_x, down_x, (1, 0), (last_x, own_y), (before_x, own_y)),
            (down_x, up_x, (-1, 0), (first_x, own_y), (after_x, own_y)),
        ]
        ends_x = {1: (one(RIM + sx - 1), one(RIM - 1)), -1: (one(RIM), one(RIM + sx))}
        ends_y = {1: (one(PAD + sy - 1), one(PAD - 1)), -1: (one(PAD), one(PAD + sy))}
        has_x = {1: (up_x, down_x), -1: (down_x, up_x)}
        has_y = {1: (up_y, down_y), -1: (down_y, up_y)}
        for i in (1, -1):
            for j in (1, -1):
                plans.append(
                    (
                        has_x[i][0] & has_y[j][0],
                        has_x[i][1] & has_y[j][1],
                        (i, j),
                        (ends_x[i][0], ends_y[j][0]),
                        (ends_x[i][1], ends_y[j][1]),
                    )
                )
        copies = []
        for k, (sends, receives, (i, j), source, target) in enumerate(plans):
            copy = pltpu.make_async_remote_copy(
                src_ref=buffer.at[(*lead, *source)],
                dst_ref=buffer.at[(*lead, *target)],
                send_sem=send_sems(k),
                recv_sem=recv_sems(k),
                device_id=(gx + i, gy + j),
                device_id_type=MESH,
            )
            copies.append((sends, receives, copy))
        return copies

    def start_rims(copies):
        for sends, _, copy in copies[4:] + copies[:4]:
            pl.when(sends)(copy.start)

    def arrived(copies):
        for _, receives, copy in copies:
            pl.when(receives)(copy.wait_recv)

    def sent(copies):
        for sends, _, copy in copies:
            pl.when(sends)(copy.wait_send)

    def start_columns(phase):
        for k in steps_x:
            to = turned(gx, k, nx)
            pltpu.make_async_remote_copy(
                src_ref=column_send.at[phase, jnp.where(to > gx, 0, 1)],
                dst_ref=column_recv.at[phase, gx],
                send_sem=col_send_sem.at[phase],
                recv_sem=col_recv_sem.at[phase],
                device_id=(to, gy),
                device_id_type=MESH,
            ).start()

    def columns_arrived(phase):
        rest = column_recv.at[phase, pl.ds(0, nx - 1)]
        pltpu.make_async_copy(rest, rest, col_recv_sem.at[phase]).wait()

    def columns_summed(phase):
        zero = jnp.zeros((sy, depth), jnp.float32)
        earlier, later = zero, zero
        for k in range(nx):
            value = column_recv[phase, k]
            earlier = earlier + jnp.where(gx > k, value, 0.0)
            later = later + jnp.where(gx < k, value, 0.0)
        return earlier, later

    lane = lax.broadcasted_iota(jnp.int32, (1, depth), 1)
    steps = far_first([(i, j) for i in range(nx) for j in range(ny) if i or j])
    others = nx * ny - 1

    def start_norms(phase, values):
        line = jnp.zeros((1, depth), jnp.float32)
        for k, value in enumerate(values):
            total = jnp.sum(jnp.sum(value, axis=0, keepdims=True), axis=1, keepdims=True)
            line = jnp.where(lane == k, total, line)
        norm_send[phase] = line
        to_x = [turned(gx, i, nx) for i in range(nx)]
        to_y = [turned(gy, j, ny) for j in range(ny)]
        for i, j in steps:
            pltpu.make_async_remote_copy(
                src_ref=norm_send.at[phase],
                dst_ref=norm_recv.at[phase, pl.ds(i * ny + j, 1)],
                send_sem=norm_send_sem.at[phase],
                recv_sem=norm_recv_sem.at[phase],
                device_id=(to_x[i], to_y[j]),
                device_id_type=MESH,
            ).start()

    def norms(phase):
        rest = norm_recv.at[phase, pl.ds(1, others)]
        pltpu.make_async_copy(rest, rest, norm_recv_sem.at[phase]).wait()
        norm_recv[phase, 0:1] = norm_send[phase]
        line = jnp.sum(norm_recv[phase], axis=0, keepdims=True)
        lines_out[phase] = line
        return steps_of(line, cells)

    loads[2].wait()
    rims = rim_copies(
        field, (pl.ds(0, 2),), lambda k: rim_send.at[0, k], lambda k: rim_recv.at[0, k]
    )
    start_rims(rims)
    start_columns(0)

    loads[4].wait()
    planes = 8
    tall = planes * sy

    def fix(step, carry):
        span = pl.ds(pl.multiple_of(step * planes, planes), planes)
        values = pobs[span].reshape(tall, depth)
        back = jnp.dot(halves(values), rev_table[...], preferred_element_type=jnp.float32)
        fixed[span] = (back * (WHOLE * zscale)).reshape(planes, sy, depth)
        pobs[span] = (values * (1.0 / zscale)).reshape(planes, sy, depth)
        return carry

    lax.fori_loop(0, sx // planes, fix, 0, unroll=2)

    long = min(LONG, sx)

    def integrate(last):
        width = (3 if last else 2) * depth
        for step in range(sx // long):
            span = pl.ds(step * long, long)
            out = jnp.dot(
                lhs[pl.ds(step * long * sy, long * sy)],
                table[:, pl.ds(0, width)],
                preferred_element_type=jnp.float32,
            )
            pulls[span] = out[:, :depth].reshape(long, sy, depth)
            slope[0, span] = out[:, depth : 2 * depth].reshape(long, sy, depth)
            if last:
                turn[span] = out[:, 2 * depth :].reshape(long, sy, depth)

    def fits():
        def body(step, squares):
            out = jnp.dot(
                lhs[pl.ds(pl.multiple_of(step * long * sy, 8), long * sy)],
                up_table[...],
                preferred_element_type=jnp.float32,
            )
            miss = out - pobs[pl.ds(step * long, long)].reshape(long * sy, depth)
            return squares + jnp.sum((miss * miss).reshape(long * sy // 8, 8, depth), axis=0)

        return lax.fori_loop(0, sx // long, body, zero_tile)

    def fill(step, values):
        lhs[pl.ds(pl.multiple_of(step * tall, tall), tall)] = halves(values.reshape(tall, depth))

    def first_fill(k, carry):
        fill(k, field[0, pl.ds(pl.multiple_of(k * planes, planes) + RIM, planes), own_y])
        return carry

    lax.fori_loop(0, sx // planes, first_fill, 0)
    integrate(False)

    def all_slopes(source, target):
        def body(step, carry):
            at = pl.multiple_of(step * planes, planes)
            target[pl.ds(at, planes)] = depth_difference(source[pl.ds(at + RIM, planes), own_y])
            return carry

        lax.fori_loop(0, sx // planes, body, 0)

    all_slopes(field.at[1], slope.at[1])

    def look_up(p, at):
        number = zone[p, at]
        low = jnp.zeros(number.shape, jnp.float32)
        high = low
        for k in range(lows.shape[0]):
            hit = number == k
            low = jnp.where(hit, low_table[k], low)
            high = jnp.where(hit, high_table[k], high)
        lower[p, at] = low
        upper[p, at] = high

    def own_look_up(x, carry):
        look_up(x + RIM, own_y)
        return carry

    def rim_look_up(x, carry):
        look_up(x + RIM, pl.ds(0, PAD))
        look_up(x + RIM, pl.ds(PAD + sy, PAD))
        return carry

    groups = sy // 8
    zero_tile = jnp.zeros((8, depth), jnp.float32)
    none = (zero_tile,) * groups

    def rows(j):
        return pl.ds(PAD + j, 8, stride=groups)

    def own(j):
        return pl.ds(j, 8, stride=groups)

    def tree(values):
        values = list(values)
        while len(values) > 1:
            values = [sum(values[k : k + 2]) for k in range(0, len(values), 2)]
        return values[0]

    ring = pl.ds(PAD - 1, 2, stride=sy + 1)
    ring_after = pl.ds(PAD, 2, stride=sy + 1)
    ring_before = pl.ds(PAD - 2, 2, stride=sy + 1)

    def edge_levers(p):
        for j in range(groups):
            first_vec, second_vec = [
                (
                    field[f, p + 1, rows(j)] - field[f, p - 1, rows(j)],
                    field[f, p, rows(j + 1)] - field[f, p, rows(j - 1)],
                    depth_difference(field[f, p, rows(j)]),
                )
                for f in range(2)
            ]
            crossed = cross(first_vec, second_vec)
            lever[0, p, rows(j)] = cross(second_vec, crossed)[0]
            lever[2, p, rows(j)] = cross(crossed, first_vec)[0]

    def plane_levers(x):
        p = x + RIM
        center = [[field[f, p, rows(j)] for j in range(-1, groups + 1)] for f in range(2)]
        squares = []
        twists = [], []
        for j in range(groups):
            first_vec, second_vec = [
                (
                    field[f, p + 1, rows(j)] - field[f, p - 1, rows(j)],
                    center[f][j + 2] - center[f][j],
                    slope[f, x, own(j)],
                )
                for f in range(2)
            ]
            crossed = cross(first_vec, second_vec)
            for f, vec in ((0, cross(second_vec, crossed)), (1, cross(crossed, first_vec))):
                lever[2 * f, p, rows(j)] = vec[0]
                lever[2 * f + 1, p, rows(j)] = vec[1]
                twists[f].append(vec[2])
            squares.append(tree([c * c for c in crossed]))
        for f in range(2):
            for j in range(0, groups, 2):
                twist_lhs[f, pl.ds(pl.multiple_of((x + BATCH) * sy, 16) + 8 * j, 16)] = halves(
                    jnp.concatenate(twists[f][j : j + 2], axis=0)
                )
        first_vec, second_vec = [
            (
                field[f, p + 1, ring] - field[f, p - 1, ring],
                field[f, p, ring_after] - field[f, p, ring_before],
                depth_difference(field[f, p, ring]),
            )
            for f in range(2)
        ]
        crossed = cross(first_vec, second_vec)
        lever[1, p, ring] = cross(second_vec, crossed)[1]
        lever[3, p, ring] = cross(crossed, first_vec)[1]
        return tree(squares)

    def untwist(x):
        for f in range(2):
            out = jnp.dot(
                twist_lhs[f, pl.ds(pl.multiple_of(x * sy, 16), BATCH * sy)],
                table[:, pl.ds(depth, depth)],
                preferred_element_type=jnp.float32,
            )
            twist[f, pl.ds(x, BATCH)] = out.reshape(BATCH, sy, depth)

    def levers(step, squares):
        x = step * BATCH
        untwist(x)
        return squares + tree([plane_levers(x + k) for k in range(BATCH)])

    def cross(u, v):
        return (u[1] * v[2] - u[2] * v[1], u[2] * v[0] - u[0] * v[2], u[0] * v[1] - u[1] * v[0])

    def spread(f, x):
        p = x + RIM
        along = [lever[2 * f + 1, p, rows(j)] for j in range(-1, groups + 1)]
        return [
            (lever[2 * f, p - 1, rows(j)] - lever[2 * f, p + 1, rows(j)])
            + ((along[j] - along[j + 2]) - twist[f, x + BATCH, pl.ds(8 * j, 8)])
            for j in range(groups)
        ]

    fit_squares = fits()
    for k in (3, 5, 6):
        loads[k].wait()
    lax.fori_loop(0, sx, own_look_up, 0)
    before = ahead = None
    rim_sets = [rims]
    for phase in range(ITERS):
        if phase == 0:
            arrived(rims)
            zone_rims = rim_copies(zone, (), lambda k: zone_send.at[k], lambda k: zone_recv.at[k])
            start_rims(zone_rims)
        none = (zero_tile,) * groups
        crossed_squares = lax.fori_loop(0, sx // BATCH, levers, zero_tile)
        edge_levers(RIM - 1)
        edge_levers(RIM + sx)
        untwist(sx)

        columns_arrived(phase)
        earlier, later = columns_summed(phase)
        if phase == 0:
            before = earlier
            ahead = (
                later * (1.0 / xscale)
                + later_parts * (before + total)
                + (weighted + float(sx) * before)
                - observed * (1.0 / xscale)
            )
        else:
            ahead = ahead - step_slowness * (
                later + later_parts * (earlier + total) + weighted + float(sx) * earlier
            )
            before = before - step_slowness * earlier

        if phase > 1:
            sent(rim_sets[phase - 1])
        slot = phase % 2

        push_scale = WHOLE * xscale * xscale

        def descend(step, carry):
            running, push_sum, total, weighted, squares = map(list, carry)
            for k in range(BATCH):
                x = step * BATCH + k
                p = x + RIM
                spreads = spread(0, x), spread(1, x)
                terms = [[] for _ in squares]
                for j in range(groups):
                    pull = (pulls[x, own(j)] - fixed[x, own(j)]) + spreads[0][j]
                    if phase < ITERS - 1:
                        grads[2 * slot, p, rows(j)] = pull
                    else:
                        pull_out[x, own(j)] = pull
                    running[j] = running[j] + field[1, p, rows(j)]
                    miss = running[j] - tobs[x, own(j)]
                    push = push_scale * push_sum[j] + spreads[1][j]
                    push_sum[j] = push_sum[j] - miss
                    if phase < ITERS - 1:
                        grads[2 * slot + 1, p, rows(j)] = push
                    else:
                        push_out[x, own(j)] = push
                    total[j] = total[j] + push
                    weighted[j] = weighted[j] + total[j]
                    values = (pull, push, miss)
                    if phase == ITERS - 1:
                        values += (turn[x, own(j)] - pobs[x, own(j)],)
                    for term, value in zip(terms, values):
                        term.append(value * value)
                squares = [square + tree(term) for square, term in zip(squares, terms)]
            return tuple(map(tuple, (running, push_sum, total, weighted, squares)))

        state[0] = before
        state[1] = ahead
        split = lambda k: tuple(state[k, own(j)] for j in range(groups))
        carry = (split(0), split(1), none, none, (zero_tile,) * (3 if phase < ITERS - 1 else 4))
        _, _, totals, weights, squares = lax.fori_loop(0, sx // BATCH, descend, carry)
        for j in range(groups):
            state[0, own(j)] = totals[j]
            state[1, own(j)] = weights[j]
        total, weighted = state[0], state[1]
        start_norms(
            phase,
            (
                squares[0],
                squares[1],
                squares[2] * (xscale * xscale)
                + crossed_squares * (1.0 / 16.0)
                + (squares[3] * (zscale * zscale) if phase == ITERS - 1 else 0.0),
                fit_squares * (zscale * zscale),
            ),
        )
        if phase < ITERS - 1:
            new_rims = rim_copies(
                grads,
                (pl.ds(2 * slot, 2),),
                lambda k, phase=phase: rim_send.at[phase + 1, k],
                lambda k, phase=phase: rim_recv.at[phase + 1, k],
            )
            rim_sets.append(new_rims)
            start_rims(new_rims)
            column_send[phase + 1, 0] = total
            column_send[phase + 1, 1] = weighted + later_parts * total
        if phase < ITERS - 1:
            all_slopes(grads.at[2 * slot + 1], turn)
            start_columns(phase + 1)
            if phase > 0:
                fit_squares = fits()
        else:

            def hand_over(x, carry):
                p = x + RIM
                density_out[x] = field[0, p, own_y]
                slowness_out[x] = field[1, p, own_y]
                lower_out[x] = lower[p, own_y]
                upper_out[x] = upper[p, own_y]
                return carry

            lax.fori_loop(0, sx, hand_over, 0, unroll=2)
        if phase == 0:
            sent(rims)
            arrived(zone_rims)
            sent(zone_rims)
            lax.fori_loop(0, sx, rim_look_up, 0, unroll=2)
            for p in (*range(RIM), *range(RIM + sx, px)):
                look_up(p, pl.ds(0, py))
        step_density, step_slowness = norms(phase)
        if phase < ITERS - 1:
            arrived(new_rims)

            def move_rim(p, at):
                d = field[0, p, at] - step_density * grads[2 * slot, p, at]
                field[0, p, at] = jnp.minimum(jnp.maximum(d, lower[p, at]), upper[p, at])
                field[1, p, at] = field[1, p, at] - step_slowness * grads[2 * slot + 1, p, at]

            for p in (*range(RIM), *range(RIM + sx, px)):
                move_rim(p, pl.ds(0, py))

            def move(step, carry):
                at = pl.multiple_of(step * planes, planes)
                span = pl.ds(at + RIM, planes)
                d = field[0, span, own_y] - step_density * grads[2 * slot, span, own_y]
                d = jnp.minimum(jnp.maximum(d, lower[span, own_y]), upper[span, own_y])
                field[0, span, own_y] = d
                fill(step, d)
                field[1, span, own_y] = (
                    field[1, span, own_y] - step_slowness * grads[2 * slot + 1, span, own_y]
                )
                slope[1, pl.ds(at, planes)] = (
                    slope[1, pl.ds(at, planes)] - step_slowness * turn[pl.ds(at, planes)]
                )
                for k in range(planes):
                    move_rim(at + RIM + k, pl.ds(0, PAD))
                    move_rim(at + RIM + k, pl.ds(PAD + sy, PAD))
                return carry

            lax.fori_loop(0, sx // planes, move, 0)
            integrate(phase == ITERS - 2)
    sent(rim_sets[-1])
    for phase in range(ITERS):
        rest = column_recv.at[phase, pl.ds(0, nx - 1)]
        pltpu.make_async_copy(rest, rest, col_send_sem.at[phase]).wait()
        rest = norm_recv.at[phase, pl.ds(1, others)]
        pltpu.make_async_copy(rest, rest, norm_send_sem.at[phase]).wait()


def solution(mesh):
    nx, ny = mesh.shape["gx"], mesh.shape["gy"]

    def local(density, slowness, pressure, times, zones, low_table, high_table):
        sx, sy, depth = density.shape
        zones_shape = low_table.shape
        px, py = sx + 2 * RIM, sy + 2 * PAD
        f32, bf16 = jnp.float32, jnp.bfloat16
        hbm = pl.BlockSpec(memory_space=pltpu.HBM)
        smem = pl.BlockSpec(memory_space=pltpu.SMEM)
        vmem = pl.BlockSpec(memory_space=pltpu.VMEM)
        dma = pltpu.SemaphoreType.DMA
        model = jax.ShapeDtypeStruct((sx, sy, depth), f32)
        inputs = (density, slowness, pressure, times, zones, low_table, high_table)
        last = pl.pallas_call(
            functools.partial(kernel, nx, ny),
            out_shape=(model,) * 6 + (jax.ShapeDtypeStruct((ITERS, 1, depth), f32),),
            in_specs=[hbm] * 7,
            out_specs=(vmem,) * 7,
            scratch_shapes=[
                pltpu.VMEM((2, px, py, depth), f32),
                pltpu.VMEM((4, px, py, depth), f32),
                pltpu.VMEM((px, py, depth), jnp.int32),
                pltpu.VMEM((px, py, depth), f32),
                pltpu.VMEM((px, py, depth), f32),
                pltpu.VMEM((4, px, py, depth), f32),
                pltpu.VMEM((2, sx + BATCH, sy, depth), f32),
                pltpu.VMEM((2, (sx + BATCH) * sy, 2 * depth), bf16),
                pltpu.VMEM((2, sx, sy, depth), f32),
                *[pltpu.VMEM((sx, sy, depth), f32)] * 5,
                pltpu.VMEM((sx * sy, 2 * depth), bf16),
                pltpu.VMEM((2 * depth, 3 * depth), bf16),
                pltpu.VMEM((2 * depth, depth), bf16),
                pltpu.VMEM((2 * depth, depth), bf16),
                pltpu.SMEM(zones_shape, f32),
                pltpu.SMEM(zones_shape, f32),
                pltpu.VMEM((ITERS, 2, sy, depth), f32),
                pltpu.VMEM((ITERS, nx, sy, depth), f32),
                pltpu.VMEM((ITERS, 1, depth), f32),
                pltpu.VMEM((ITERS, nx * ny, depth), f32),
                dma((7,)),
                dma((ITERS, 8)),
                dma((ITERS, 8)),
                dma((8,)),
                dma((8,)),
                dma((ITERS,)),
                dma((ITERS,)),
                dma((ITERS,)),
                dma((ITERS,)),
                pltpu.VMEM((2, sy, depth), f32),
            ],
            compiler_params=pltpu.CompilerParams(
                collective_id=0,
                has_side_effects=True,
                vmem_limit_bytes=44 * 1024 * 1024,
            ),
        )(*[pltpu.with_memory_space_constraint(value, pltpu.HBM) for value in inputs])
        return pl.pallas_call(
            functools.partial(finish, float(nx * sx * ny * sy * depth)),
            out_shape=(model, model, jax.ShapeDtypeStruct((ITERS,), f32)),
            in_specs=[vmem] * 7,
            out_specs=(pl.BlockSpec(memory_space=pl.ANY),) * 2 + (smem,),
            scratch_shapes=[
                pltpu.VMEM((sx, sy, depth), f32),
                pltpu.VMEM((sx, sy, depth), f32),
                dma((16,)),
            ],
            compiler_params=pltpu.CompilerParams(vmem_limit_bytes=8 * 1024 * 1024),
        )(*last)

    part = P("gx", "gy", None)
    return jax.shard_map(
        local,
        mesh=mesh,
        in_specs=(part,) * 5 + (P(), P()),
        out_specs=(part, part, P()),
        check_vma=False,
    )
```

```python
import functools
import math

import jax
import jax.numpy as jnp
from jax import lax
from jax.experimental import pallas as pl
from jax.experimental.pallas import tpu as pltpu
from jax.sharding import PartitionSpec as P

ITERS = 3
ETA = 0.5
EPSILON = 1e-06
MESH = pl.DeviceIdType.MESH
PAD = 8
RIM = 2
LONG = 32
WHOLE = 16.0
BATCH = 8


def depth_difference(values):
    lane = lax.broadcasted_iota(jnp.int32, values.shape, values.ndim - 1)
    last = values.shape[-1] - 1
    after = pltpu.roll(values, last, values.ndim - 1)
    before = pltpu.roll(values, 1, values.ndim - 1)
    return jnp.where(lane == last, 0.0, after) - jnp.where(lane == 0, 0.0, before)


def halves(values):
    high = values.astype(jnp.bfloat16)
    low = (values - high.astype(jnp.float32)).astype(jnp.bfloat16)
    return jnp.concatenate([high, low], axis=-1)


def steps_of(line, cells):
    lane = lax.broadcasted_iota(jnp.int32, line.shape, 1)
    scale = 1.0 / (WHOLE * WHOLE * cells)
    norm = lambda k: jnp.sum(jnp.where(lane == k, line, 0.0), axis=1, keepdims=True) * scale
    return [(ETA / WHOLE) * lax.rsqrt(norm(k) + EPSILON) for k in range(2)]


def finish(
    cells,
    density,
    pull,
    lower,
    upper,
    slowness,
    push,
    lines,
    density_out,
    slowness_out,
    objective,
    density_new,
    slowness_new,
    history,
    sem,
):
    step_density, step_slowness = steps_of(lines[ITERS - 1], cells)
    pieces = 8
    length = density.shape[0] // pieces
    pairs = ((density_new, density_out, sem.at[0]), (slowness_new, slowness_out, sem.at[1]))
    for k in range(pieces):
        span = pl.ds(k * length, length)

        def body(x, carry):
            moved = density[x] - step_density * pull[x]
            density_new[x] = jnp.minimum(jnp.maximum(moved, lower[x]), upper[x])
            slowness_new[x] = slowness[x] - step_slowness * push[x]
            return carry

        lax.fori_loop(k * length, (k + 1) * length, body, 0, unroll=2)
        for source, target, done in pairs:
            pltpu.make_async_copy(source.at[span], target.at[span], done).start()
    lane = lax.broadcasted_iota(jnp.int32, (1, lines.shape[-1]), 1)
    pick = lambda phase, k: jnp.where(lane == k, lines[phase], 0.0)
    for phase in range(ITERS):
        parts = pick(phase, 2)
        if phase < ITERS - 1:
            parts = parts + pick(phase + 1, 3)
        history[phase] = jnp.sum(parts) * (0.5 / cells)
    copy = pltpu.make_async_copy(history, objective, sem.at[2])
    copy.start()
    for source, target, done in pairs:
        pltpu.make_async_copy(source, target, done).wait()
    copy.wait()


def kernel(
    nx,
    ny,
    density,
    slowness,
    pressure,
    times,
    zones,
    lows,
    highs,
    density_out,
    pull_out,
    lower_out,
    upper_out,
    slowness_out,
    push_out,
    lines_out,
    field,
    grads,
    zone,
    lower,
    upper,
    lever,
    twist,
    twist_lhs,
    kept,
    slope,
    turn,
    pulls,
    fixed,
    pobs,
    tobs,
    lhs,
    table,
    rev_table,
    up_table,
    low_table,
    high_table,
    column_send,
    column_recv,
    norm_send,
    norm_recv,
    load_sem,
    rim_send,
    rim_recv,
    zone_recv,
    col_send_sem,
    col_recv_sem,
    norm_send_sem,
    norm_recv_sem,
    state,
):
    sx, sy, depth = density.shape
    px, py = sx + 2 * RIM, sy + 2 * PAD
    cells = float(nx * sx * ny * sy * depth)
    zscale = 1.0 / math.sqrt(depth)
    xscale = 1.0 / math.sqrt(nx * sx)
    gx, gy = lax.axis_index("gx"), lax.axis_index("gy")
    own_x, own_y = pl.ds(RIM, sx), pl.ds(PAD, sy)

    loads = [
        pltpu.make_async_copy(slowness, field.at[1, own_x, own_y], load_sem.at[0]),
        pltpu.make_async_copy(times, tobs, load_sem.at[1]),
        pltpu.make_async_copy(density, field.at[0, own_x, own_y], load_sem.at[2]),
        pltpu.make_async_copy(zones, zone.at[own_x, own_y], load_sem.at[3]),
        pltpu.make_async_copy(pressure, pobs, load_sem.at[4]),
        pltpu.make_async_copy(lows, low_table, load_sem.at[5]),
        pltpu.make_async_copy(highs, high_table, load_sem.at[6]),
    ]
    for copy in loads:
        copy.start()

    def turned(value, step, size):
        return lax.rem(value + step, size)

    near = [0, 1, 2, 1]

    def far_first(steps):
        if (nx, ny) == (16, 8):
            steps = sorted(steps, key=lambda t: -(near[t[0] // 4] + near[t[0] % 4] + near[t[1] // 2]))
        return steps

    barrier = pltpu.get_barrier_semaphore()
    steps_x = [i for i, _ in far_first([(i, 0) for i in range(1, nx)])]
    greet = [(i, 0) for i in range(1, nx)] + [(0, j) for j in range(1, ny)]
    greet += [(i, j) for i in (1, nx - 1) for j in (1, ny - 1)]
    for i, j in far_first(greet):
        device = (turned(gx, i, nx), turned(gy, j, ny))
        pl.semaphore_signal(barrier, inc=1, device_id=device, device_id_type=MESH)

    @pl.when(gy == 0)
    def _():
        for buffer in (field, grads):
            buffer[:, :, 0:PAD] = jnp.zeros((buffer.shape[0], px, PAD, depth), jnp.float32)

    @pl.when(gy == ny - 1)
    def _():
        for buffer in (field, grads):
            buffer[:, :, PAD + sy :] = jnp.zeros((buffer.shape[0], px, PAD, depth), jnp.float32)

    @pl.when(gx == 0)
    def _():
        for buffer in (field, grads):
            buffer[:, 0:RIM] = jnp.zeros((buffer.shape[0], RIM, py, depth), jnp.float32)

    @pl.when(gx == nx - 1)
    def _():
        for buffer in (field, grads):
            buffer[:, RIM + sx :] = jnp.zeros((buffer.shape[0], RIM, py, depth), jnp.float32)

    row = lax.broadcasted_iota(jnp.int32, (depth, depth), 0)
    col = lax.broadcasted_iota(jnp.int32, (depth, depth), 1)
    upward = jnp.where(row <= col, 1.0, 0.0).astype(jnp.bfloat16)
    both = ((depth - jnp.maximum(row, col)).astype(jnp.float32) * (WHOLE / depth)).astype(jnp.bfloat16)
    differ = (jnp.where(row == col + 1, 1.0, 0.0) - jnp.where(row == col - 1, 1.0, 0.0)).astype(jnp.bfloat16)
    downward = jnp.where(row >= col, 1.0, 0.0).astype(jnp.bfloat16)
    for half in range(2):
        tall = pl.ds(half * depth, depth)
        table[tall, pl.ds(0, depth)] = both
        table[tall, pl.ds(depth, depth)] = differ
        table[tall, pl.ds(2 * depth, depth)] = upward
        up_table[tall, :] = upward
        rev_table[tall, :] = downward

    loads[0].wait()
    loads[1].wait()

    def first_sums(x, carry):
        running, weighted, observed = carry
        running = running + field[1, x + RIM, own_y]
        seen = tobs[x]
        tobs[x] = seen * (1.0 / xscale)
        return running, weighted + running, observed + seen

    zero = jnp.zeros((sy, depth), jnp.float32)
    total, weighted, observed = lax.fori_loop(0, sx, first_sums, (zero, zero, zero), unroll=4)
    later_parts = (nx - 1 - gx).astype(jnp.float32) * float(sx)
    column_send[0, 0] = total
    column_send[0, 1] = xscale * (weighted + later_parts * total) - observed
    pl.semaphore_wait(barrier, len(greet))

    def rim_copies(buffer, lead, send_sems, recv_sems):
        first_x, last_x = pl.ds(RIM, RIM), pl.ds(RIM + sx - RIM, RIM)
        before_x, after_x = pl.ds(0, RIM), pl.ds(RIM + sx, RIM)
        first_y, last_y = pl.ds(PAD, RIM), pl.ds(PAD + sy - RIM, RIM)
        before_y, after_y = pl.ds(PAD - RIM, RIM), pl.ds(PAD + sy, RIM)
        one = lambda at: pl.ds(at, 1)
        up_x, down_x, up_y, down_y = gx < nx - 1, gx > 0, gy < ny - 1, gy > 0
        plans = [
            (up_y, down_y, (0, 1), (own_x, last_y), (own_x, before_y)),
            (down_y, up_y, (0, -1), (own_x, first_y), (own_x, after_y)),
            (up_x, down_x, (1, 0), (last_x, own_y), (before_x, own_y)),
            (down_x, up_x, (-1, 0), (first_x, own_y), (after_x, own_y)),
        ]
        ends_x = {1: (one(RIM + sx - 1), one(RIM - 1)), -1: (one(RIM), one(RIM + sx))}
        ends_y = {1: (one(PAD + sy - 1), one(PAD - 1)), -1: (one(PAD), one(PAD + sy))}
        has_x = {1: (up_x, down_x), -1: (down_x, up_x)}
        has_y = {1: (up_y, down_y), -1: (down_y, up_y)}
        for i in (1, -1):
            for j in (1, -1):
                plans.append(
                    (
                        has_x[i][0] & has_y[j][0],
                        has_x[i][1] & has_y[j][1],
                        (i, j),
                        (ends_x[i][0], ends_y[j][0]),
                        (ends_x[i][1], ends_y[j][1]),
                    )
                )
        copies = []
        for k, (sends, receives, (i, j), source, target) in enumerate(plans):
            copy = pltpu.make_async_remote_copy(
                src_ref=buffer.at[(*lead, *source)],
                dst_ref=buffer.at[(*lead, *target)],
                send_sem=send_sems(k),
                recv_sem=recv_sems(k),
                device_id=(gx + i, gy + j),
                device_id_type=MESH,
            )
            copies.append((sends, receives, copy))
        return copies

    def start_rims(copies):
        for sends, _, copy in copies[4:] + copies[:4]:
            pl.when(sends)(copy.start)

    def arrived(copies):
        for _, receives, copy in copies:
            pl.when(receives)(copy.wait_recv)

    def sent(copies):
        for sends, _, copy in copies:
            pl.when(sends)(copy.wait_send)

    def start_columns(phase):
        for k in steps_x:
            to = turned(gx, k, nx)
            pltpu.make_async_remote_copy(
                src_ref=column_send.at[phase, jnp.where(to > gx, 0, 1)],
                dst_ref=column_recv.at[phase, gx],
                send_sem=col_send_sem,
                recv_sem=col_recv_sem.at[phase % 2],
                device_id=(to, gy),
                device_id_type=MESH,
            ).start()

    def columns_arrived(phase):
        rest = column_recv.at[phase, pl.ds(0, nx - 1)]
        pltpu.make_async_copy(rest, rest, col_recv_sem.at[phase % 2]).wait()
        pltpu.make_async_copy(rest, rest, col_send_sem).wait()

    def columns_summed(phase):
        zero = jnp.zeros((sy, depth), jnp.float32)
        earlier, later = zero, zero
        for k in range(nx):
            value = column_recv[phase, k]
            earlier = earlier + jnp.where(gx > k, value, 0.0)
            later = later + jnp.where(gx < k, value, 0.0)
        return earlier, later

    lane = lax.broadcasted_iota(jnp.int32, (1, depth), 1)
    steps = far_first([(i, j) for i in range(nx) for j in range(ny) if i or j])
    others = nx * ny - 1

    def start_norms(phase, values):
        line = jnp.zeros((1, depth), jnp.float32)
        for k, value in enumerate(values):
            total = jnp.sum(jnp.sum(value, axis=0, keepdims=True), axis=1, keepdims=True)
            line = jnp.where(lane == k, total, line)
        norm_send[phase] = line
        to_x = [turned(gx, i, nx) for i in range(nx)]
        to_y = [turned(gy, j, ny) for j in range(ny)]
        for i, j in steps:
            pltpu.make_async_remote_copy(
                src_ref=norm_send.at[phase],
                dst_ref=norm_recv.at[phase, pl.ds(i * ny + j, 1)],
                send_sem=norm_send_sem,
                recv_sem=norm_recv_sem.at[phase % 2],
                device_id=(to_x[i], to_y[j]),
                device_id_type=MESH,
            ).start()

    def norms(phase):
        rest = norm_recv.at[phase, pl.ds(1, others)]
        pltpu.make_async_copy(rest, rest, norm_recv_sem.at[phase % 2]).wait()
        pltpu.make_async_copy(rest, rest, norm_send_sem).wait()
        norm_recv[phase, 0:1] = norm_send[phase]
        line = jnp.sum(norm_recv[phase], axis=0, keepdims=True)
        lines_out[phase] = line
        return steps_of(line, cells)

    loads[2].wait()
    rims = rim_copies(
        field, (pl.ds(0, 2),), lambda k: rim_send.at[k], lambda k: rim_recv.at[0, k]
    )
    start_rims(rims)
    start_columns(0)

    loads[4].wait()
    planes = 8
    tall = planes * sy

    def fix(step, carry):
        span = pl.ds(pl.multiple_of(step * planes, planes), planes)
        values = pobs[span].reshape(tall, depth)
        back = jnp.dot(halves(values), rev_table[...], preferred_element_type=jnp.float32)
        fixed[span] = (back * (WHOLE * zscale)).reshape(planes, sy, depth)
        pobs[span] = (values * (1.0 / zscale)).reshape(planes, sy, depth)
        return carry

    lax.fori_loop(0, sx // planes, fix, 0, unroll=2)

    long = min(LONG, sx)

    def integrate(last):
        width = (3 if last else 2) * depth
        for step in range(sx // long):
            span = pl.ds(step * long, long)
            out = jnp.dot(
                lhs[pl.ds(step * long * sy, long * sy)],
                table[:, pl.ds(0, width)],
                preferred_element_type=jnp.float32,
            )
            pulls[span] = out[:, :depth].reshape(long, sy, depth)
            slope[0, span] = out[:, depth : 2 * depth].reshape(long, sy, depth)
            if last:
                turn[span] = out[:, 2 * depth :].reshape(long, sy, depth)

    def fits():
        def body(step, squares):
            out = jnp.dot(
                lhs[pl.ds(pl.multiple_of(step * long * sy, 8), long * sy)],
                up_table[...],
                preferred_element_type=jnp.float32,
            )
            miss = out - pobs[pl.ds(step * long, long)].reshape(long * sy, depth)
            return squares + jnp.sum((miss * miss).reshape(long * sy // 8, 8, depth), axis=0)

        return lax.fori_loop(0, sx // long, body, zero_tile)

    def fill(step, values):
        lhs[pl.ds(pl.multiple_of(step * tall, tall), tall)] = halves(values.reshape(tall, depth))

    def first_fill(k, carry):
        fill(k, field[0, pl.ds(pl.multiple_of(k * planes, planes) + RIM, planes), own_y])
        return carry

    lax.fori_loop(0, sx // planes, first_fill, 0)
    integrate(False)

    def all_slopes(source, target):
        def body(step, carry):
            at = pl.multiple_of(step * planes, planes)
            target[pl.ds(at, planes)] = depth_difference(source[pl.ds(at + RIM, planes), own_y])
            return carry

        lax.fori_loop(0, sx // planes, body, 0)

    all_slopes(field.at[1], slope.at[1])

    def look_up(p, at):
        number = zone[p, at]
        low = jnp.zeros(number.shape, jnp.float32)
        high = low
        for k in range(lows.shape[0]):
            hit = number == k
            low = jnp.where(hit, low_table[k], low)
            high = jnp.where(hit, high_table[k], high)
        lower[p, at] = low
        upper[p, at] = high

    def own_look_up(x, carry):
        look_up(x + RIM, own_y)
        return carry

    def rim_look_up(x, carry):
        look_up(x + RIM, pl.ds(0, PAD))
        look_up(x + RIM, pl.ds(PAD + sy, PAD))
        return carry

    groups = sy // 8
    zero_tile = jnp.zeros((8, depth), jnp.float32)
    none = (zero_tile,) * groups

    def rows(j):
        return pl.ds(PAD + j, 8, stride=groups)

    def own(j):
        return pl.ds(j, 8, stride=groups)

    def tree(values):
        values = list(values)
        while len(values) > 1:
            values = [sum(values[k : k + 2]) for k in range(0, len(values), 2)]
        return values[0]

    ring = pl.ds(PAD - 1, 2, stride=sy + 1)
    ring_after = pl.ds(PAD, 2, stride=sy + 1)
    ring_before = pl.ds(PAD - 2, 2, stride=sy + 1)

    def edge_levers(p):
        for j in range(groups):
            first_vec, second_vec = [
                (
                    field[f, p + 1, rows(j)] - field[f, p - 1, rows(j)],
                    field[f, p, rows(j + 1)] - field[f, p, rows(j - 1)],
                    depth_difference(field[f, p, rows(j)]),
                )
                for f in range(2)
            ]
            crossed = cross(first_vec, second_vec)
            lever[0, p, rows(j)] = cross(second_vec, crossed)[0]
            lever[2, p, rows(j)] = cross(crossed, first_vec)[0]

    def plane_levers(x, last):
        p = x + RIM
        center = [[field[f, p, rows(j)] for j in range(-1, groups + 1)] for f in range(2)]
        squares = []
        twists = [], []
        for j in range(groups):
            first_vec, second_vec = [
                (
                    field[f, p + 1, rows(j)] - field[f, p - 1, rows(j)],
                    center[f][j + 2] - center[f][j],
                    slope[f, x, own(j)],
                )
                for f in range(2)
            ]
            crossed = cross(first_vec, second_vec)
            for f, vec in ((0, cross(second_vec, crossed)), (1, cross(crossed, first_vec))):
                lever[2 * f, p, rows(j)] = vec[0]
                lever[2 * f + 1, p, rows(j)] = vec[1]
                twists[f].append(vec[2])
            if last:
                squares.append(tree([c * c for c in crossed]))
            else:
                for k, value in enumerate(crossed):
                    kept[k, x, pl.ds(8 * j, 8)] = value
        for f in range(2):
            for j in range(0, groups, 2):
                twist_lhs[f, pl.ds(pl.multiple_of((x + BATCH) * sy, 16) + 8 * j, 16)] = halves(
                    jnp.concatenate(twists[f][j : j + 2], axis=0)
                )
        first_vec, second_vec = [
            (
                field[f, p + 1, ring] - field[f, p - 1, ring],
                field[f, p, ring_after] - field[f, p, ring_before],
                depth_difference(field[f, p, ring]),
            )
            for f in range(2)
        ]
        crossed = cross(first_vec, second_vec)
        lever[1, p, ring] = cross(second_vec, crossed)[1]
        lever[3, p, ring] = cross(crossed, first_vec)[1]
        return tree(squares) if last else None

    def untwist(x):
        for f in range(2):
            out = jnp.dot(
                twist_lhs[f, pl.ds(pl.multiple_of(x * sy, 16), BATCH * sy)],
                table[:, pl.ds(depth, depth)],
                preferred_element_type=jnp.float32,
            )
            twist[f, pl.ds(x, BATCH)] = out.reshape(BATCH, sy, depth)

    def levers(last, step, squares):
        x = step * BATCH
        untwist(x)
        parts = [plane_levers(x + k, last) for k in range(BATCH)]
        return squares + tree(parts) if last else squares

    def cross(u, v):
        return (u[1] * v[2] - u[2] * v[1], u[2] * v[0] - u[0] * v[2], u[0] * v[1] - u[1] * v[0])

    def kept_squares():
        def body(step, squares):
            x = step * 4
            sums = [
                tree([jnp.sum((kept[k, x + i] ** 2).reshape(sy // 8, 8, depth), axis=0) for i in range(4)])
                for k in range(3)
            ]
            return squares + tree(sums)

        return lax.fori_loop(0, sx // 4, body, zero_tile)

    def spread(f, x):
        p = x + RIM
        along = [lever[2 * f + 1, p, rows(j)] for j in range(-1, groups + 1)]
        return [
            (lever[2 * f, p - 1, rows(j)] - lever[2 * f, p + 1, rows(j)])
            + ((along[j] - along[j + 2]) - twist[f, x + BATCH, pl.ds(8 * j, 8)])
            for j in range(groups)
        ]

    late_parts = zero_tile
    loads[3].wait()
    before = ahead = None
    rim_sets = [rims]
    for phase in range(ITERS):
        if phase == 0:
            arrived(rims)
            sent(rims)
            zone_rims = rim_copies(zone, (), lambda k: rim_send.at[k], lambda k: zone_recv.at[k])
            start_rims(zone_rims)
        none = (zero_tile,) * groups
        crossed_squares = lax.fori_loop(
            0, sx // BATCH, functools.partial(levers, phase == ITERS - 1), zero_tile
        )
        edge_levers(RIM - 1)
        edge_levers(RIM + sx)
        untwist(sx)

        columns_arrived(phase)
        earlier, later = columns_summed(phase)
        if phase == 0:
            before = earlier
            ahead = (
                later * (1.0 / xscale)
                + later_parts * (before + total)
                + (weighted + float(sx) * before)
                - observed * (1.0 / xscale)
            )
        else:
            ahead = ahead - step_slowness * (
                later + later_parts * (earlier + total) + weighted + float(sx) * earlier
            )
            before = before - step_slowness * earlier

        if phase == 0:
            sent(zone_rims)
        else:
            sent(rim_sets[phase])
        slot = phase % 2

        push_scale = WHOLE * xscale * xscale

        def descend(step, carry):
            running, push_sum, total, weighted, squares = map(list, carry)
            for k in range(BATCH):
                x = step * BATCH + k
                p = x + RIM
                spreads = spread(0, x), spread(1, x)
                terms = [[] for _ in squares]
                for j in range(groups):
                    pull = (pulls[x, own(j)] - fixed[x, own(j)]) + spreads[0][j]
                    if phase < ITERS - 1:
                        grads[2 * slot, p, rows(j)] = pull
                    else:
                        pull_out[x, own(j)] = pull
                    running[j] = running[j] + field[1, p, rows(j)]
                    miss = running[j] - tobs[x, own(j)]
                    push = push_scale * push_sum[j] + spreads[1][j]
                    push_sum[j] = push_sum[j] - miss
                    if phase < ITERS - 1:
                        grads[2 * slot + 1, p, rows(j)] = push
                    else:
                        push_out[x, own(j)] = push
                    total[j] = total[j] + push
                    weighted[j] = weighted[j] + total[j]
                    values = (pull, push, miss)
                    if phase == ITERS - 1:
                        values += (turn[x, own(j)] - pobs[x, own(j)],)
                    for term, value in zip(terms, values):
                        term.append(value * value)
                squares = [square + tree(term) for square, term in zip(squares, terms)]
            return tuple(map(tuple, (running, push_sum, total, weighted, squares)))

        state[0] = before
        state[1] = ahead
        split = lambda k: tuple(state[k, own(j)] for j in range(groups))
        carry = (split(0), split(1), none, none, (zero_tile,) * (3 if phase < ITERS - 1 else 4))
        _, _, totals, weights, squares = lax.fori_loop(0, sx // BATCH, descend, carry)
        for j in range(groups):
            state[0, own(j)] = totals[j]
            state[1, own(j)] = weights[j]
        total, weighted = state[0], state[1]
        start_norms(
            phase,
            (
                squares[0],
                squares[1],
                squares[2] * (xscale * xscale)
                + crossed_squares * (1.0 / 16.0)
                + (squares[3] * (zscale * zscale) if phase == ITERS - 1 else 0.0),
                late_parts,
            ),
        )
        if phase < ITERS - 1:
            new_rims = rim_copies(
                grads,
                (pl.ds(2 * slot, 2),),
                lambda k: rim_send.at[k],
                lambda k, phase=phase: rim_recv.at[(phase + 1) % 2, k],
            )
            rim_sets.append(new_rims)
            start_rims(new_rims)
            column_send[phase + 1, 0] = total
            column_send[phase + 1, 1] = weighted + later_parts * total
        if phase < ITERS - 1:
            all_slopes(grads.at[2 * slot + 1], turn)
            start_columns(phase + 1)
            late_parts = fits() * (zscale * zscale) + kept_squares() * (1.0 / 16.0)
        else:

            def hand_over(x, carry):
                p = x + RIM
                density_out[x] = field[0, p, own_y]
                slowness_out[x] = field[1, p, own_y]
                lower_out[x] = lower[p, own_y]
                upper_out[x] = upper[p, own_y]
                return carry

            lax.fori_loop(0, sx, hand_over, 0, unroll=2)
        if phase == 0:
            loads[5].wait()
            loads[6].wait()
            lax.fori_loop(0, sx, own_look_up, 0)
            arrived(zone_rims)
            lax.fori_loop(0, sx, rim_look_up, 0, unroll=2)
            for p in (*range(RIM), *range(RIM + sx, px)):
                look_up(p, pl.ds(0, py))
        step_density, step_slowness = norms(phase)
        if phase < ITERS - 1:
            arrived(new_rims)

            def move_rim(p, at):
                d = field[0, p, at] - step_density * grads[2 * slot, p, at]
                field[0, p, at] = jnp.minimum(jnp.maximum(d, lower[p, at]), upper[p, at])
                field[1, p, at] = field[1, p, at] - step_slowness * grads[2 * slot + 1, p, at]

            for p in (*range(RIM), *range(RIM + sx, px)):
                move_rim(p, pl.ds(0, py))

            def move(step, carry):
                at = pl.multiple_of(step * planes, planes)
                span = pl.ds(at + RIM, planes)
                d = field[0, span, own_y] - step_density * grads[2 * slot, span, own_y]
                d = jnp.minimum(jnp.maximum(d, lower[span, own_y]), upper[span, own_y])
                field[0, span, own_y] = d
                fill(step, d)
                field[1, span, own_y] = (
                    field[1, span, own_y] - step_slowness * grads[2 * slot + 1, span, own_y]
                )
                slope[1, pl.ds(at, planes)] = (
                    slope[1, pl.ds(at, planes)] - step_slowness * turn[pl.ds(at, planes)]
                )
                for k in range(planes):
                    move_rim(at + RIM + k, pl.ds(0, PAD))
                    move_rim(at + RIM + k, pl.ds(PAD + sy, PAD))
                return carry

            lax.fori_loop(0, sx // planes, move, 0)
            integrate(phase == ITERS - 2)


def solution(mesh):
    nx, ny = mesh.shape["gx"], mesh.shape["gy"]

    def local(density, slowness, pressure, times, zones, low_table, high_table):
        sx, sy, depth = density.shape
        zones_shape = low_table.shape
        px, py = sx + 2 * RIM, sy + 2 * PAD
        f32, bf16 = jnp.float32, jnp.bfloat16
        hbm = pl.BlockSpec(memory_space=pltpu.HBM)
        vmem = pl.BlockSpec(memory_space=pltpu.VMEM)
        dma = pltpu.SemaphoreType.DMA
        model = jax.ShapeDtypeStruct((sx, sy, depth), f32)
        inputs = (density, slowness, pressure, times, zones, low_table, high_table)
        last = pl.pallas_call(
            functools.partial(kernel, nx, ny),
            out_shape=(model,) * 6 + (jax.ShapeDtypeStruct((ITERS, 1, depth), f32),),
            in_specs=[hbm] * 7,
            out_specs=(vmem,) * 7,
            scratch_shapes=[
                pltpu.VMEM((2, px, py, depth), f32),
                pltpu.VMEM((4, px, py, depth), f32),
                pltpu.VMEM((px, py, depth), jnp.int32),
                pltpu.VMEM((px, py, depth), f32),
                pltpu.VMEM((px, py, depth), f32),
                pltpu.VMEM((4, px, py, depth), f32),
                pltpu.VMEM((2, sx + BATCH, sy, depth), f32),
                pltpu.VMEM((2, (sx + BATCH) * sy, 2 * depth), bf16),
                pltpu.VMEM((3, sx, sy, depth), f32),
                pltpu.VMEM((2, sx, sy, depth), f32),
                *[pltpu.VMEM((sx, sy, depth), f32)] * 5,
                pltpu.VMEM((sx * sy, 2 * depth), bf16),
                pltpu.VMEM((2 * depth, 3 * depth), bf16),
                pltpu.VMEM((2 * depth, depth), bf16),
                pltpu.VMEM((2 * depth, depth), bf16),
                pltpu.SMEM(zones_shape, f32),
                pltpu.SMEM(zones_shape, f32),
                pltpu.VMEM((ITERS, 2, sy, depth), f32),
                pltpu.VMEM((ITERS, nx, sy, depth), f32),
                pltpu.VMEM((ITERS, 1, depth), f32),
                pltpu.VMEM((ITERS, nx * ny, depth), f32),
                dma((7,)),
                dma((8,)),
                dma((2, 8)),
                dma((8,)),
                dma,
                dma((2,)),
                dma,
                dma((2,)),
                pltpu.VMEM((2, sy, depth), f32),
            ],
            compiler_params=pltpu.CompilerParams(
                collective_id=0,
                has_side_effects=True,
                vmem_limit_bytes=46 * 1024 * 1024,
            ),
        )(*[pltpu.with_memory_space_constraint(value, pltpu.HBM) for value in inputs])
        return pl.pallas_call(
            functools.partial(finish, float(nx * sx * ny * sy * depth)),
            out_shape=(model, model, jax.ShapeDtypeStruct((ITERS,), f32)),
            in_specs=[vmem] * 7,
            out_specs=(pl.BlockSpec(memory_space=pl.ANY),) * 3,
            scratch_shapes=[
                pltpu.VMEM((sx, sy, depth), f32),
                pltpu.VMEM((sx, sy, depth), f32),
                pltpu.SMEM((ITERS,), f32),
                dma((3,)),
            ],
            compiler_params=pltpu.CompilerParams(vmem_limit_bytes=8 * 1024 * 1024),
        )(*last)

    part = P("gx", "gy", None)
    return jax.shard_map(
        local,
        mesh=mesh,
        in_specs=(part,) * 5 + (P(), P()),
        out_specs=(part, part, P()),
        check_vma=False,
    )
```

```python
import functools
import math

import jax
import jax.numpy as jnp
from jax import lax
from jax.experimental import pallas as pl
from jax.experimental.pallas import tpu as pltpu
from jax.sharding import PartitionSpec as P

ITERS = 3
ETA = 0.5
EPSILON = 1e-06
MESH = pl.DeviceIdType.MESH
PAD = 8
RIM = 2
LONG = 32
WHOLE = 16.0
BATCH = 8


def depth_difference(values):
    lane = lax.broadcasted_iota(jnp.int32, values.shape, values.ndim - 1)
    last = values.shape[-1] - 1
    after = pltpu.roll(values, last, values.ndim - 1)
    before = pltpu.roll(values, 1, values.ndim - 1)
    return jnp.where(lane == last, 0.0, after) - jnp.where(lane == 0, 0.0, before)


def halves(values):
    high = values.astype(jnp.bfloat16)
    low = (values - high.astype(jnp.float32)).astype(jnp.bfloat16)
    return jnp.concatenate([high, low], axis=-1)


def steps_of(line, cells):
    lane = lax.broadcasted_iota(jnp.int32, line.shape, 1)
    scale = 1.0 / (WHOLE * WHOLE * cells)
    norm = lambda k: jnp.sum(jnp.where(lane == k, line, 0.0), axis=1, keepdims=True) * scale
    return [(ETA / WHOLE) * lax.rsqrt(norm(k) + EPSILON) for k in range(2)]


def finish(
    cells,
    density,
    pull,
    lower,
    upper,
    slowness,
    push,
    lines,
    density_out,
    slowness_out,
    objective,
    density_new,
    slowness_new,
    history,
    sem,
):
    step_density, step_slowness = steps_of(lines[ITERS - 1], cells)
    pieces = 8
    length = density.shape[0] // pieces
    pairs = ((density_new, density_out, sem.at[0]), (slowness_new, slowness_out, sem.at[1]))
    for k in range(pieces):
        span = pl.ds(k * length, length)

        def body(x, carry):
            moved = density[x] - step_density * pull[x]
            density_new[x] = jnp.minimum(jnp.maximum(moved, lower[x]), upper[x])
            slowness_new[x] = slowness[x] - step_slowness * push[x]
            return carry

        lax.fori_loop(k * length, (k + 1) * length, body, 0, unroll=4)
        for source, target, done in pairs:
            pltpu.make_async_copy(source.at[span], target.at[span], done).start()
    lane = lax.broadcasted_iota(jnp.int32, (1, lines.shape[-1]), 1)
    pick = lambda phase, k: jnp.where(lane == k, lines[phase], 0.0)
    for phase in range(ITERS):
        parts = pick(phase, 2)
        if phase < ITERS - 1:
            parts = parts + pick(phase + 1, 3)
        history[phase] = jnp.sum(parts) * (0.5 / cells)
    copy = pltpu.make_async_copy(history, objective, sem.at[2])
    copy.start()
    for source, target, done in pairs:
        pltpu.make_async_copy(source, target, done).wait()
    copy.wait()


def kernel(
    nx,
    ny,
    density,
    slowness,
    pressure,
    times,
    zones,
    lows,
    highs,
    density_out,
    pull_out,
    lower_out,
    upper_out,
    slowness_out,
    push_out,
    lines_out,
    field,
    grads,
    zone,
    lower,
    upper,
    lever,
    twist,
    twist_lhs,
    kept,
    slope,
    turn,
    pulls,
    fixed,
    pobs,
    tobs,
    lhs,
    table,
    rev_table,
    up_table,
    low_table,
    high_table,
    column_send,
    column_recv,
    norm_send,
    norm_recv,
    load_sem,
    rim_send,
    rim_recv,
    zone_recv,
    col_send_sem,
    col_recv_sem,
    norm_send_sem,
    norm_recv_sem,
    state,
):
    sx, sy, depth = density.shape
    px, py = sx + 2 * RIM, sy + 2 * PAD
    cells = float(nx * sx * ny * sy * depth)
    zscale = 1.0 / math.sqrt(depth)
    xscale = 1.0 / math.sqrt(nx * sx)
    gx, gy = lax.axis_index("gx"), lax.axis_index("gy")
    own_x, own_y = pl.ds(RIM, sx), pl.ds(PAD, sy)

    loads = [
        pltpu.make_async_copy(slowness, field.at[1, own_x, own_y], load_sem.at[0]),
        pltpu.make_async_copy(times, tobs, load_sem.at[1]),
        pltpu.make_async_copy(density, field.at[0, own_x, own_y], load_sem.at[2]),
        pltpu.make_async_copy(zones, zone.at[own_x, own_y], load_sem.at[3]),
        pltpu.make_async_copy(pressure, pobs, load_sem.at[4]),
        pltpu.make_async_copy(lows, low_table, load_sem.at[5]),
        pltpu.make_async_copy(highs, high_table, load_sem.at[6]),
    ]
    for copy in loads:
        copy.start()

    def turned(value, step, size):
        return lax.rem(value + step, size)

    near = [0, 1, 2, 1]

    def far_first(steps):
        if (nx, ny) == (16, 8):
            steps = sorted(steps, key=lambda t: -(near[t[0] // 4] + near[t[0] % 4] + near[t[1] // 2]))
        return steps

    barrier = pltpu.get_barrier_semaphore()
    steps_x = [i for i, _ in far_first([(i, 0) for i in range(1, nx)])]
    greet = [(i, 0) for i in range(1, nx)] + [(0, j) for j in range(1, ny)]
    greet += [(i, j) for i in (1, nx - 1) for j in (1, ny - 1)]
    for i, j in far_first(greet):
        device = (turned(gx, i, nx), turned(gy, j, ny))
        pl.semaphore_signal(barrier, inc=1, device_id=device, device_id_type=MESH)

    @pl.when(gy == 0)
    def _():
        for buffer in (field, grads):
            buffer[:, :, 0:PAD] = jnp.zeros((buffer.shape[0], px, PAD, depth), jnp.float32)

    @pl.when(gy == ny - 1)
    def _():
        for buffer in (field, grads):
            buffer[:, :, PAD + sy :] = jnp.zeros((buffer.shape[0], px, PAD, depth), jnp.float32)

    @pl.when(gx == 0)
    def _():
        for buffer in (field, grads):
            buffer[:, 0:RIM] = jnp.zeros((buffer.shape[0], RIM, py, depth), jnp.float32)

    @pl.when(gx == nx - 1)
    def _():
        for buffer in (field, grads):
            buffer[:, RIM + sx :] = jnp.zeros((buffer.shape[0], RIM, py, depth), jnp.float32)

    row = lax.broadcasted_iota(jnp.int32, (depth, depth), 0)
    col = lax.broadcasted_iota(jnp.int32, (depth, depth), 1)
    upward = jnp.where(row <= col, 1.0, 0.0).astype(jnp.bfloat16)
    both = ((depth - jnp.maximum(row, col)).astype(jnp.float32) * (WHOLE / depth)).astype(jnp.bfloat16)
    differ = (jnp.where(row == col + 1, 1.0, 0.0) - jnp.where(row == col - 1, 1.0, 0.0)).astype(jnp.bfloat16)
    downward = jnp.where(row >= col, 1.0, 0.0).astype(jnp.bfloat16)
    for half in range(2):
        tall = pl.ds(half * depth, depth)
        table[tall, pl.ds(0, depth)] = both
        table[tall, pl.ds(depth, depth)] = differ
        table[tall, pl.ds(2 * depth, depth)] = upward
        up_table[tall, :] = upward
        rev_table[tall, :] = downward

    loads[0].wait()
    loads[1].wait()

    def first_sums(x, carry):
        running, weighted, observed = carry
        running = running + field[1, x + RIM, own_y]
        seen = tobs[x]
        tobs[x] = seen * (1.0 / xscale)
        return running, weighted + running, observed + seen

    zero = jnp.zeros((sy, depth), jnp.float32)
    total, weighted, observed = lax.fori_loop(0, sx, first_sums, (zero, zero, zero), unroll=4)
    later_parts = (nx - 1 - gx).astype(jnp.float32) * float(sx)
    column_send[0, 0] = total
    column_send[0, 1] = xscale * (weighted + later_parts * total) - observed
    pl.semaphore_wait(barrier, len(greet))

    def rim_copies(buffer, lead, send_sems, recv_sems):
        first_x, last_x = pl.ds(RIM, RIM), pl.ds(RIM + sx - RIM, RIM)
        before_x, after_x = pl.ds(0, RIM), pl.ds(RIM + sx, RIM)
        first_y, last_y = pl.ds(PAD, RIM), pl.ds(PAD + sy - RIM, RIM)
        before_y, after_y = pl.ds(PAD - RIM, RIM), pl.ds(PAD + sy, RIM)
        one = lambda at: pl.ds(at, 1)
        up_x, down_x, up_y, down_y = gx < nx - 1, gx > 0, gy < ny - 1, gy > 0
        plans = [
            (up_y, down_y, (0, 1), (own_x, last_y), (own_x, before_y)),
            (down_y, up_y, (0, -1), (own_x, first_y), (own_x, after_y)),
            (up_x, down_x, (1, 0), (last_x, own_y), (before_x, own_y)),
            (down_x, up_x, (-1, 0), (first_x, own_y), (after_x, own_y)),
        ]
        ends_x = {1: (one(RIM + sx - 1), one(RIM - 1)), -1: (one(RIM), one(RIM + sx))}
        ends_y = {1: (one(PAD + sy - 1), one(PAD - 1)), -1: (one(PAD), one(PAD + sy))}
        has_x = {1: (up_x, down_x), -1: (down_x, up_x)}
        has_y = {1: (up_y, down_y), -1: (down_y, up_y)}
        for i in (1, -1):
            for j in (1, -1):
                plans.append(
                    (
                        has_x[i][0] & has_y[j][0],
                        has_x[i][1] & has_y[j][1],
                        (i, j),
                        (ends_x[i][0], ends_y[j][0]),
                        (ends_x[i][1], ends_y[j][1]),
                    )
                )
        copies = []
        for k, (sends, receives, (i, j), source, target) in enumerate(plans):
            copy = pltpu.make_async_remote_copy(
                src_ref=buffer.at[(*lead, *source)],
                dst_ref=buffer.at[(*lead, *target)],
                send_sem=send_sems(k),
                recv_sem=recv_sems(k),
                device_id=(gx + i, gy + j),
                device_id_type=MESH,
            )
            copies.append((sends, receives, copy))
        return copies

    def start_rims(copies):
        for sends, _, copy in copies[4:] + copies[:4]:
            pl.when(sends)(copy.start)

    def arrived(copies):
        for _, receives, copy in copies:
            pl.when(receives)(copy.wait_recv)

    def sent(copies):
        for sends, _, copy in copies:
            pl.when(sends)(copy.wait_send)

    def start_columns(phase):
        for k in steps_x:
            to = turned(gx, k, nx)
            pltpu.make_async_remote_copy(
                src_ref=column_send.at[phase, jnp.where(to > gx, 0, 1)],
                dst_ref=column_recv.at[phase, gx],
                send_sem=col_send_sem,
                recv_sem=col_recv_sem.at[phase % 2],
                device_id=(to, gy),
                device_id_type=MESH,
            ).start()

    def columns_arrived(phase):
        rest = column_recv.at[phase, pl.ds(0, nx - 1)]
        pltpu.make_async_copy(rest, rest, col_recv_sem.at[phase % 2]).wait()
        pltpu.make_async_copy(rest, rest, col_send_sem).wait()

    def columns_summed(phase):
        zero = jnp.zeros((sy, depth), jnp.float32)
        earlier, later = zero, zero
        for k in range(nx):
            value = column_recv[phase, k]
            earlier = earlier + jnp.where(gx > k, value, 0.0)
            later = later + jnp.where(gx < k, value, 0.0)
        return earlier, later

    lane = lax.broadcasted_iota(jnp.int32, (1, depth), 1)
    steps = far_first([(i, j) for i in range(nx) for j in range(ny) if i or j])
    others = nx * ny - 1

    def start_norms(phase, values):
        line = jnp.zeros((1, depth), jnp.float32)
        for k, value in enumerate(values):
            total = jnp.sum(jnp.sum(value, axis=0, keepdims=True), axis=1, keepdims=True)
            line = jnp.where(lane == k, total, line)
        norm_send[phase] = line
        to_x = [turned(gx, i, nx) for i in range(nx)]
        to_y = [turned(gy, j, ny) for j in range(ny)]
        for i, j in steps:
            pltpu.make_async_remote_copy(
                src_ref=norm_send.at[phase],
                dst_ref=norm_recv.at[phase, pl.ds(i * ny + j, 1)],
                send_sem=norm_send_sem,
                recv_sem=norm_recv_sem.at[phase % 2],
                device_id=(to_x[i], to_y[j]),
                device_id_type=MESH,
            ).start()

    def norms(phase):
        rest = norm_recv.at[phase, pl.ds(1, others)]
        pltpu.make_async_copy(rest, rest, norm_recv_sem.at[phase % 2]).wait()
        pltpu.make_async_copy(rest, rest, norm_send_sem).wait()
        norm_recv[phase, 0:1] = norm_send[phase]
        line = jnp.sum(norm_recv[phase], axis=0, keepdims=True)
        lines_out[phase] = line
        return steps_of(line, cells)

    loads[2].wait()
    rims = rim_copies(
        field, (pl.ds(0, 2),), lambda k: rim_send.at[k], lambda k: rim_recv.at[0, k]
    )
    start_rims(rims)
    start_columns(0)

    loads[4].wait()
    planes = 8
    tall = planes * sy

    def fix(step, carry):
        span = pl.ds(pl.multiple_of(step * planes, planes), planes)
        values = pobs[span].reshape(tall, depth)
        back = jnp.dot(halves(values), rev_table[...], preferred_element_type=jnp.float32)
        fixed[span] = (back * (WHOLE * zscale)).reshape(planes, sy, depth)
        pobs[span] = (values * (1.0 / zscale)).reshape(planes, sy, depth)
        return carry

    lax.fori_loop(0, sx // planes, fix, 0, unroll=2)

    long = min(LONG, sx)

    def integrate(last):
        width = (3 if last else 2) * depth
        for step in range(sx // long):
            span = pl.ds(step * long, long)
            out = jnp.dot(
                lhs[pl.ds(step * long * sy, long * sy)],
                table[:, pl.ds(0, width)],
                preferred_element_type=jnp.float32,
            )
            pulls[span] = out[:, :depth].reshape(long, sy, depth)
            slope[0, span] = out[:, depth : 2 * depth].reshape(long, sy, depth)
            if last:
                turn[span] = out[:, 2 * depth :].reshape(long, sy, depth)

    def fits():
        def body(step, squares):
            out = jnp.dot(
                lhs[pl.ds(pl.multiple_of(step * long * sy, 8), long * sy)],
                up_table[...],
                preferred_element_type=jnp.float32,
            )
            miss = out - pobs[pl.ds(step * long, long)].reshape(long * sy, depth)
            return squares + jnp.sum((miss * miss).reshape(long * sy // 8, 8, depth), axis=0)

        return lax.fori_loop(0, sx // long, body, zero_tile)

    def fill(step, values):
        lhs[pl.ds(pl.multiple_of(step * tall, tall), tall)] = halves(values.reshape(tall, depth))

    def first_fill(k, carry):
        fill(k, field[0, pl.ds(pl.multiple_of(k * planes, planes) + RIM, planes), own_y])
        return carry

    lax.fori_loop(0, sx // planes, first_fill, 0)
    integrate(False)

    def all_slopes(source, target):
        def body(step, carry):
            at = pl.multiple_of(step * planes, planes)
            target[pl.ds(at, planes)] = depth_difference(source[pl.ds(at + RIM, planes), own_y])
            return carry

        lax.fori_loop(0, sx // planes, body, 0)

    all_slopes(field.at[1], slope.at[1])

    def look_up(p, at):
        number = zone[p, at]
        low = jnp.zeros(number.shape, jnp.float32)
        high = low
        for k in range(lows.shape[0]):
            hit = number == k
            low = jnp.where(hit, low_table[k], low)
            high = jnp.where(hit, high_table[k], high)
        lower[p, at] = low
        upper[p, at] = high

    def own_look_up(x, carry):
        look_up(x + RIM, own_y)
        return carry

    def rim_look_up(x, carry):
        look_up(x + RIM, pl.ds(0, PAD))
        look_up(x + RIM, pl.ds(PAD + sy, PAD))
        return carry

    groups = sy // 8
    zero_tile = jnp.zeros((8, depth), jnp.float32)
    none = (zero_tile,) * groups

    def rows(j):
        return pl.ds(PAD + j, 8, stride=groups)

    def own(j):
        return pl.ds(j, 8, stride=groups)

    def tree(values):
        values = list(values)
        while len(values) > 1:
            values = [sum(values[k : k + 2]) for k in range(0, len(values), 2)]
        return values[0]

    ring = pl.ds(PAD - 1, 2, stride=sy + 1)
    ring_after = pl.ds(PAD, 2, stride=sy + 1)
    ring_before = pl.ds(PAD - 2, 2, stride=sy + 1)

    def edge_levers(p):
        for j in range(groups):
            first_vec, second_vec = [
                (
                    field[f, p + 1, rows(j)] - field[f, p - 1, rows(j)],
                    field[f, p, rows(j + 1)] - field[f, p, rows(j - 1)],
                    depth_difference(field[f, p, rows(j)]),
                )
                for f in range(2)
            ]
            crossed = cross(first_vec, second_vec)
            lever[0, p, rows(j)] = cross(second_vec, crossed)[0]
            lever[2, p, rows(j)] = cross(crossed, first_vec)[0]

    def plane_levers(x, last):
        p = x + RIM
        center = [[field[f, p, rows(j)] for j in range(-1, groups + 1)] for f in range(2)]
        squares = []
        twists = [], []
        for j in range(groups):
            first_vec, second_vec = [
                (
                    field[f, p + 1, rows(j)] - field[f, p - 1, rows(j)],
                    center[f][j + 2] - center[f][j],
                    slope[f, x, own(j)],
                )
                for f in range(2)
            ]
            crossed = cross(first_vec, second_vec)
            for f, vec in ((0, cross(second_vec, crossed)), (1, cross(crossed, first_vec))):
                lever[2 * f, p, rows(j)] = vec[0]
                lever[2 * f + 1, p, rows(j)] = vec[1]
                twists[f].append(vec[2])
            if last:
                squares.append(tree([c * c for c in crossed]))
            else:
                for k, value in enumerate(crossed):
                    kept[k, x, pl.ds(8 * j, 8)] = value
        for f in range(2):
            for j in range(0, groups, 2):
                twist_lhs[f, pl.ds(pl.multiple_of((x + BATCH) * sy, 16) + 8 * j, 16)] = halves(
                    jnp.concatenate(twists[f][j : j + 2], axis=0)
                )
        first_vec, second_vec = [
            (
                field[f, p + 1, ring] - field[f, p - 1, ring],
                field[f, p, ring_after] - field[f, p, ring_before],
                depth_difference(field[f, p, ring]),
            )
            for f in range(2)
        ]
        crossed = cross(first_vec, second_vec)
        lever[1, p, ring] = cross(second_vec, crossed)[1]
        lever[3, p, ring] = cross(crossed, first_vec)[1]
        return tree(squares) if last else None

    def untwist(x):
        for f in range(2):
            out = jnp.dot(
                twist_lhs[f, pl.ds(pl.multiple_of(x * sy, 16), BATCH * sy)],
                table[:, pl.ds(depth, depth)],
                preferred_element_type=jnp.float32,
            )
            twist[f, pl.ds(x, BATCH)] = out.reshape(BATCH, sy, depth)

    def levers(last, step, squares):
        x = step * BATCH
        untwist(x)
        parts = [plane_levers(x + k, last) for k in range(BATCH)]
        return squares + tree(parts) if last else squares

    def cross(u, v):
        return (u[1] * v[2] - u[2] * v[1], u[2] * v[0] - u[0] * v[2], u[0] * v[1] - u[1] * v[0])

    def kept_squares():
        def body(step, squares):
            x = step * 4
            sums = [
                tree([jnp.sum((kept[k, x + i] ** 2).reshape(sy // 8, 8, depth), axis=0) for i in range(4)])
                for k in range(3)
            ]
            return squares + tree(sums)

        return lax.fori_loop(0, sx // 4, body, zero_tile)

    def spread(f, x):
        p = x + RIM
        along = [lever[2 * f + 1, p, rows(j)] for j in range(-1, groups + 1)]
        return [
            (lever[2 * f, p - 1, rows(j)] - lever[2 * f, p + 1, rows(j)])
            + ((along[j] - along[j + 2]) - twist[f, x + BATCH, pl.ds(8 * j, 8)])
            for j in range(groups)
        ]

    late_parts = zero_tile
    loads[3].wait()
    before = ahead = None
    rim_sets = [rims]
    for phase in range(ITERS):
        if phase == 0:
            arrived(rims)
            sent(rims)
            zone_rims = rim_copies(zone, (), lambda k: rim_send.at[k], lambda k: zone_recv.at[k])
            start_rims(zone_rims)
        none = (zero_tile,) * groups
        crossed_squares = lax.fori_loop(
            0, sx // BATCH, functools.partial(levers, phase == ITERS - 1), zero_tile
        )
        edge_levers(RIM - 1)
        edge_levers(RIM + sx)
        untwist(sx)

        columns_arrived(phase)
        earlier, later = columns_summed(phase)
        if phase == 0:
            before = earlier
            ahead = (
                later * (1.0 / xscale)
                + later_parts * (before + total)
                + (weighted + float(sx) * before)
                - observed * (1.0 / xscale)
            )
        else:
            ahead = ahead - step_slowness * (
                later + later_parts * (earlier + total) + weighted + float(sx) * earlier
            )
            before = before - step_slowness * earlier

        if phase == 0:
            sent(zone_rims)
        else:
            sent(rim_sets[phase])
        slot = phase % 2

        push_scale = WHOLE * xscale * xscale

        def descend(step, carry):
            running, push_sum, total, weighted, squares = map(list, carry)
            for k in range(BATCH):
                x = step * BATCH + k
                p = x + RIM
                spreads = spread(0, x), spread(1, x)
                terms = [[] for _ in squares]
                for j in range(groups):
                    pull = (pulls[x, own(j)] - fixed[x, own(j)]) + spreads[0][j]
                    if phase < ITERS - 1:
                        grads[2 * slot, p, rows(j)] = pull
                    else:
                        pull_out[x, own(j)] = pull
                    running[j] = running[j] + field[1, p, rows(j)]
                    miss = running[j] - tobs[x, own(j)]
                    push = push_scale * push_sum[j] + spreads[1][j]
                    push_sum[j] = push_sum[j] - miss
                    if phase < ITERS - 1:
                        grads[2 * slot + 1, p, rows(j)] = push
                    else:
                        push_out[x, own(j)] = push
                    total[j] = total[j] + push
                    weighted[j] = weighted[j] + total[j]
                    values = (pull, push, miss)
                    if phase == ITERS - 1:
                        values += (turn[x, own(j)] - pobs[x, own(j)],)
                    for term, value in zip(terms, values):
                        term.append(value * value)
                squares = [square + tree(term) for square, term in zip(squares, terms)]
            return tuple(map(tuple, (running, push_sum, total, weighted, squares)))

        state[0] = before
        state[1] = ahead
        split = lambda k: tuple(state[k, own(j)] for j in range(groups))
        carry = (split(0), split(1), none, none, (zero_tile,) * (3 if phase < ITERS - 1 else 4))
        _, _, totals, weights, squares = lax.fori_loop(0, sx // BATCH, descend, carry)
        for j in range(groups):
            state[0, own(j)] = totals[j]
            state[1, own(j)] = weights[j]
        total, weighted = state[0], state[1]
        start_norms(
            phase,
            (
                squares[0],
                squares[1],
                squares[2] * (xscale * xscale)
                + crossed_squares * (1.0 / 16.0)
                + (squares[3] * (zscale * zscale) if phase == ITERS - 1 else 0.0),
                late_parts,
            ),
        )
        if phase < ITERS - 1:
            new_rims = rim_copies(
                grads,
                (pl.ds(2 * slot, 2),),
                lambda k: rim_send.at[k],
                lambda k, phase=phase: rim_recv.at[(phase + 1) % 2, k],
            )
            rim_sets.append(new_rims)
            start_rims(new_rims)
            column_send[phase + 1, 0] = total
            column_send[phase + 1, 1] = weighted + later_parts * total
        if phase < ITERS - 1:
            all_slopes(grads.at[2 * slot + 1], turn)
            start_columns(phase + 1)
            late_parts = fits() * (zscale * zscale) + kept_squares() * (1.0 / 16.0)
        else:

            def hand_over(x, carry):
                p = x + RIM
                density_out[x] = field[0, p, own_y]
                slowness_out[x] = field[1, p, own_y]
                lower_out[x] = lower[p, own_y]
                upper_out[x] = upper[p, own_y]
                return carry

            lax.fori_loop(0, sx, hand_over, 0, unroll=2)
        if phase == 0:
            loads[5].wait()
            loads[6].wait()
            lax.fori_loop(0, sx, own_look_up, 0)
            arrived(zone_rims)
            lax.fori_loop(0, sx, rim_look_up, 0, unroll=2)
            for p in (*range(RIM), *range(RIM + sx, px)):
                look_up(p, pl.ds(0, py))
        step_density, step_slowness = norms(phase)
        if phase < ITERS - 1:
            arrived(new_rims)

            def move_rim(p, at):
                d = field[0, p, at] - step_density * grads[2 * slot, p, at]
                field[0, p, at] = jnp.minimum(jnp.maximum(d, lower[p, at]), upper[p, at])
                field[1, p, at] = field[1, p, at] - step_slowness * grads[2 * slot + 1, p, at]

            for p in (*range(RIM), *range(RIM + sx, px)):
                move_rim(p, pl.ds(0, py))

            def move(step, carry):
                at = pl.multiple_of(step * planes, planes)
                span = pl.ds(at + RIM, planes)
                d = field[0, span, own_y] - step_density * grads[2 * slot, span, own_y]
                d = jnp.minimum(jnp.maximum(d, lower[span, own_y]), upper[span, own_y])
                field[0, span, own_y] = d
                fill(step, d)
                field[1, span, own_y] = (
                    field[1, span, own_y] - step_slowness * grads[2 * slot + 1, span, own_y]
                )
                slope[1, pl.ds(at, planes)] = (
                    slope[1, pl.ds(at, planes)] - step_slowness * turn[pl.ds(at, planes)]
                )
                for k in range(planes):
                    move_rim(at + RIM + k, pl.ds(0, PAD))
                    move_rim(at + RIM + k, pl.ds(PAD + sy, PAD))
                return carry

            lax.fori_loop(0, sx // planes, move, 0)
            integrate(phase == ITERS - 2)


def solution(mesh):
    nx, ny = mesh.shape["gx"], mesh.shape["gy"]

    def local(density, slowness, pressure, times, zones, low_table, high_table):
        sx, sy, depth = density.shape
        zones_shape = low_table.shape
        px, py = sx + 2 * RIM, sy + 2 * PAD
        f32, bf16 = jnp.float32, jnp.bfloat16
        hbm = pl.BlockSpec(memory_space=pltpu.HBM)
        vmem = pl.BlockSpec(memory_space=pltpu.VMEM)
        dma = pltpu.SemaphoreType.DMA
        model = jax.ShapeDtypeStruct((sx, sy, depth), f32)
        inputs = (density, slowness, pressure, times, zones, low_table, high_table)
        last = pl.pallas_call(
            functools.partial(kernel, nx, ny),
            out_shape=(model,) * 6 + (jax.ShapeDtypeStruct((ITERS, 1, depth), f32),),
            in_specs=[hbm] * 7,
            out_specs=(vmem,) * 7,
            scratch_shapes=[
                pltpu.VMEM((2, px, py, depth), f32),
                pltpu.VMEM((4, px, py, depth), f32),
                pltpu.VMEM((px, py, depth), jnp.int32),
                pltpu.VMEM((px, py, depth), f32),
                pltpu.VMEM((px, py, depth), f32),
                pltpu.VMEM((4, px, py, depth), f32),
                pltpu.VMEM((2, sx + BATCH, sy, depth), f32),
                pltpu.VMEM((2, (sx + BATCH) * sy, 2 * depth), bf16),
                pltpu.VMEM((3, sx, sy, depth), f32),
                pltpu.VMEM((2, sx, sy, depth), f32),
                *[pltpu.VMEM((sx, sy, depth), f32)] * 5,
                pltpu.VMEM((sx * sy, 2 * depth), bf16),
                pltpu.VMEM((2 * depth, 3 * depth), bf16),
                pltpu.VMEM((2 * depth, depth), bf16),
                pltpu.VMEM((2 * depth, depth), bf16),
                pltpu.SMEM(zones_shape, f32),
                pltpu.SMEM(zones_shape, f32),
                pltpu.VMEM((ITERS, 2, sy, depth), f32),
                pltpu.VMEM((ITERS, nx, sy, depth), f32),
                pltpu.VMEM((ITERS, 1, depth), f32),
                pltpu.VMEM((ITERS, nx * ny, depth), f32),
                dma((7,)),
                dma((8,)),
                dma((2, 8)),
                dma((8,)),
                dma,
                dma((2,)),
                dma,
                dma((2,)),
                pltpu.VMEM((2, sy, depth), f32),
            ],
            compiler_params=pltpu.CompilerParams(
                collective_id=0,
                has_side_effects=True,
                vmem_limit_bytes=46 * 1024 * 1024,
            ),
        )(*[pltpu.with_memory_space_constraint(value, pltpu.HBM) for value in inputs])
        return pl.pallas_call(
            functools.partial(finish, float(nx * sx * ny * sy * depth)),
            out_shape=(model, model, jax.ShapeDtypeStruct((ITERS,), f32)),
            in_specs=[vmem] * 7,
            out_specs=(pl.BlockSpec(memory_space=pl.ANY),) * 3,
            scratch_shapes=[
                pltpu.VMEM((sx, sy, depth), f32),
                pltpu.VMEM((sx, sy, depth), f32),
                pltpu.SMEM((ITERS,), f32),
                dma((3,)),
            ],
            compiler_params=pltpu.CompilerParams(vmem_limit_bytes=8 * 1024 * 1024),
        )(*last)

    part = P("gx", "gy", None)
    return jax.shard_map(
        local,
        mesh=mesh,
        in_specs=(part,) * 5 + (P(), P()),
        out_specs=(part, part, P()),
        check_vma=False,
    )
```
